128 devices in a mesh: aa: 8 (over x, core), ba: 16 (over z, y).
Axes of the slice: x: 4, y: 4, z: 4, core: 2. Of those that a mesh axis runs over, the one named last changes fastest.
Arguments:
- initial_dictionary_matrix: bfloat16 [65536, 3584], P('ba', 'aa'), may hold values from -60 to 60
- decoder_two: bfloat16 [65536, 3584], P('ba', 'aa'), may hold values from -60 to 60
- route_one: int32 [16, 16], replicated, may hold values from 0 to 7
- route_two: int32 [16, 16], replicated, may hold values from 0 to 7
- candidate_pair_slots: int32 [16, 24, 2], P('ba'), may hold values from 0 to 15
Outputs:
- leading_logarithmic_factor: float32 [65536], P('ba')
- col_log_scale: float32 [65536], P('ba')
The draws below stay inside these ranges and needn't reach their ends.
All inputs are finite; a program needn't handle non-finite values.
Results may differ from the reference program's by a relative error of at most 0.00046.
Values may be sent and summed in bfloat16 or wider, within the bound.
No kernel may reach another device: no remote copies, remote signals or barrier semaphores. Data moves between devices by JAX's collectives and lax.ppermute only.
A program may use at most 128 MiB of HBM per device.

```python
import math
import jax
import jax.numpy as jnp
from jax import lax

D = 3584
BS = 512
PAIRS_COL = 24
SWEEPS = 4
NF = 65536
BLK_DEV = 8
NBLK = 128
N_BA = 16


def draw_decoder(key, count, width):
    key_scale, key_body = jax.random.split(key, 2)
    scales = jnp.exp(jax.random.uniform(key_scale, (count, 1), jnp.float32, 0.0, math.log(10.0)))
    values = jnp.clip(jax.random.normal(key_body, (count, width), jnp.float32), -6.0, 6.0)
    return (scales * values).astype(jnp.bfloat16)


def pairing_plan(key):
    folded_result = jax.random.fold_in(key, 101)
    key_first, key_second, key_pairs = jax.random.split(folded_result, 3)
    route_one = jax.random.randint(key_first, (N_BA, N_BA), 0, BLK_DEV, jnp.int32)
    route_two = jax.random.randint(key_second, (N_BA, N_BA), 0, BLK_DEV, jnp.int32)
    candidate_pair_slots = jax.random.randint(key_pairs, (N_BA, PAIRS_COL, 2), 0, N_BA, jnp.int32)
    return (route_one, route_two, candidate_pair_slots)


def draw_route_one(key, part):
    return pairing_plan(key)[0]


def draw_route_two(key, part):
    return pairing_plan(key)[1]


def draw_candidate_pair_slots(key, part):
    return pairing_plan(key)[2]


def draw_initial_dictionary_matrix(key, part):
    return draw_decoder(jax.random.fold_in(key, 11), NF, D)


def draw_decoder_two(key, part):
    source_rows = draw_decoder(jax.random.fold_in(key, 11), NF, D).astype(jnp.float32)
    fresh_rows = draw_decoder(jax.random.fold_in(key, 23), NF, D).astype(jnp.float32)
    route_one, route_two, candidate_pair_slots = pairing_plan(key)
    owners = jnp.broadcast_to(jnp.arange(N_BA, dtype=jnp.int32)[:, None], (N_BA, PAIRS_COL))
    source_one = candidate_pair_slots[:, :, 0]
    source_two = candidate_pair_slots[:, :, 1]
    row_block = (source_one * BLK_DEV + route_one[source_one, owners]).reshape(-1).astype(jnp.int32)
    col_block = (source_two * BLK_DEV + route_two[source_two, owners]).reshape(-1).astype(jnp.int32)
    pair_count = row_block.shape[0]
    pair_index = jnp.arange(pair_count, dtype=jnp.int32)
    matches = col_block[None, :] == jnp.arange(NBLK, dtype=jnp.int32)[:, None]
    earliest = jnp.min(jnp.where(matches, pair_index[None, :], pair_count), axis=1)
    present = earliest < pair_count
    partner = row_block[jnp.minimum(earliest, pair_count - 1)]
    key_pick, key_place, key_intersection = jax.random.split(jax.random.fold_in(key, 37), 3)
    row_ids = jnp.arange(NF, dtype=jnp.int32)
    block_of = row_ids // BS
    chosen = jnp.logical_and(present[block_of], jax.random.uniform(key_pick, (NF,), jnp.float32) < 0.25)
    selected_entry_line = partner[block_of] * BS + jax.random.randint(key_place, (NF,), 0, BS, jnp.int32)
    intersection = jax.random.uniform(key_intersection, (NF, 1), jnp.float32, 0.5, 0.95)
    target = source_rows[selected_entry_line]
    target = target / jnp.sqrt(jnp.sum(target * target, axis=1, keepdims=True) + 1e-12)
    projection = jnp.sum(fresh_rows * target, axis=1, keepdims=True)
    across = fresh_rows - projection * target
    length = jnp.sqrt(jnp.sum(fresh_rows * fresh_rows, axis=1, keepdims=True))
    across = across * (length / jnp.sqrt(jnp.sum(across * across, axis=1, keepdims=True) + 1e-12))
    planted_matching = intersection * length * target + jnp.sqrt(1.0 - intersection * intersection) * across
    values = jnp.where(chosen[:, None], planted_matching, fresh_rows)
    return jnp.clip(values, -60.0, 60.0).astype(jnp.bfloat16)


def setup_inputs(seed: int = 0) -> dict:
    key_list = jax.random.split(jax.random.key(seed), 6)
    return {
        "initial_dictionary_matrix": draw_initial_dictionary_matrix(jax.random.fold_in(key_list[5], 71), 0),
        "decoder_two": draw_decoder_two(jax.random.fold_in(key_list[5], 71), 0),
        "route_one": draw_route_one(jax.random.fold_in(key_list[5], 71), 0),
        "route_two": draw_route_two(jax.random.fold_in(key_list[5], 71), 0),
        "candidate_pair_slots": draw_candidate_pair_slots(jax.random.fold_in(key_list[5], 71), 0),
    }


smoothing_regularizer = 0.02
norm_floor = 1e-06

def unit_rows(decoder):
    widened = decoder.astype(jnp.float32)
    squares = lax.optimization_barrier(jnp.sum(widened * widened, axis=1, keepdims=True))
    return (widened * lax.rsqrt(squares + norm_floor)).astype(jnp.bfloat16)

def reference(initial_dictionary_matrix, decoder_two, route_one, route_two, candidate_pair_slots):
    unit_one = unit_rows(initial_dictionary_matrix).reshape(NBLK, BS, D)
    unit_two = unit_rows(decoder_two).reshape(NBLK, BS, D)
    owners = jnp.broadcast_to(jnp.arange(N_BA, dtype=jnp.int32)[:, None], (N_BA, PAIRS_COL))
    source_one = candidate_pair_slots[:, :, 0]
    source_two = candidate_pair_slots[:, :, 1]
    row_block = (source_one * BLK_DEV + route_one[source_one, owners]).reshape(-1).astype(jnp.int32)
    col_block = (source_two * BLK_DEV + route_two[source_two, owners]).reshape(-1).astype(jnp.int32)

    def kernel_of(blocks):
        angular_agreement = jnp.dot(unit_one[blocks[0]], unit_two[blocks[1]].T, preferred_element_type=jnp.float32)
        return jnp.exp(angular_agreement / smoothing_regularizer)
    exponential_affinity = lax.map(kernel_of, (row_block, col_block))
    col_scale = jnp.ones((NBLK, BS), jnp.float32)
    row_scale = jnp.ones((NBLK, BS), jnp.float32)
    for sweep_index in range(SWEEPS):
        row_terms = jnp.einsum('pij,pj->pi', exponential_affinity, col_scale[col_block], precision=lax.Precision.HIGHEST)
        row_scale = 1.0 / (1.0 + jax.ops.segment_sum(row_terms, row_block, num_segments=NBLK))
        col_terms = jnp.einsum('pij,pi->pj', exponential_affinity, row_scale[row_block], precision=lax.Precision.HIGHEST)
        col_scale = 1.0 / (1.0 + jax.ops.segment_sum(col_terms, col_block, num_segments=NBLK))
    return (jnp.log(row_scale).reshape(NF), jnp.log(col_scale).reshape(NF))
```

```python
import functools

import jax
import jax.numpy as jnp
from jax import lax
from jax.experimental import pallas as pl
from jax.experimental.pallas import tpu as pltpu
from jax.sharding import Mesh
from jax.sharding import PartitionSpec as P

BS = 512
SWEEPS = 4
BA = ("ba_0", "ba_1")
AA = ("aa_0", "aa_1")
ALL = AA + BA
LANES = 128
TILES = BS // LANES
HALF = BS // 2
FIXED = 32000.0
IDS = 16

smoothing_regularizer = 0.02
norm_floor = 1e-06

f32, bf16, i16, i32 = jnp.float32, jnp.bfloat16, jnp.int16, jnp.int32


def call(kernel, out_shape, grid_spec, flops, bytes_accessed, args):
    return pl.pallas_call(
        kernel,
        out_shape=out_shape,
        grid_spec=grid_spec,
        compiler_params=pltpu.CompilerParams(vmem_limit_bytes=24 * 2**20),
        cost_estimate=pl.CostEstimate(
            flops=flops, bytes_accessed=bytes_accessed, transcendentals=0
        ),
    )(*args)


def pack_first_kernel(one_ref, two_ref, a_ref, b_ref, inv_a_ref, inv_b_ref, out_ref):
    out_ref[0, :, :BS] = (b_ref[...].astype(f32) * inv_b_ref[...]).astype(bf16)
    out_ref[0, :, BS:] = (a_ref[...].astype(f32) * inv_a_ref[...]).astype(bf16)


def pack_second_kernel(one_ref, a_ref, inv_a_ref, ids_ref, out_ref):
    width = a_ref.shape[0]
    out_ref[0, :width, :] = (a_ref[...].astype(f32) * inv_a_ref[...]).astype(bf16)
    out_ref[0, width:, :] = ids_ref[...]


def pack_first(one, two, a, b, inv_a, inv_b):
    width, owners = a.shape[0], one.shape[0]
    spec = pltpu.PrefetchScalarGridSpec(
        num_scalar_prefetch=2,
        grid=(owners,),
        in_specs=[
            pl.BlockSpec((width, HALF), lambda o, r1, r2: (0, 2 * r1[o])),
            pl.BlockSpec((width, BS), lambda o, r1, r2: (0, r2[o])),
            pl.BlockSpec((1, HALF), lambda o, r1, r2: (0, 2 * r1[o])),
            pl.BlockSpec((1, BS), lambda o, r1, r2: (0, r2[o])),
        ],
        out_specs=pl.BlockSpec((1, width, BS + HALF), lambda o, r1, r2: (o, 0, 0)),
    )
    shape = jax.ShapeDtypeStruct((owners, width, BS + HALF), bf16)
    size = owners * width * (BS + HALF)
    return call(
        pack_first_kernel, shape, spec, 2 * size, 4 * size, (one, two, a, b, inv_a, inv_b)
    )


def pack_second(one, a, inv_a, ids):
    width, owners = a.shape[0], one.shape[0]
    spec = pltpu.PrefetchScalarGridSpec(
        num_scalar_prefetch=1,
        grid=(owners,),
        in_specs=[
            pl.BlockSpec((width, HALF), lambda o, r1: (0, 2 * r1[o] + 1)),
            pl.BlockSpec((1, HALF), lambda o, r1: (0, 2 * r1[o] + 1)),
            pl.BlockSpec((IDS, HALF), lambda o, r1: (0, 0)),
        ],
        out_specs=pl.BlockSpec((1, width + IDS, HALF), lambda o, r1: (o, 0, 0)),
    )
    shape = jax.ShapeDtypeStruct((owners, width + IDS, HALF), bf16)
    size = owners * width * HALF
    return call(pack_second_kernel, shape, spec, 2 * size, 4 * size, (one, a, inv_a, ids))


def cosine_kernel(s_ref, r_ref, a_ref, b_ref, out_ref):
    partial = lax.dot_general(
        a_ref[0], b_ref[0], (((0,), (0,)), ((), ())), preferred_element_type=f32
    )
    out_ref[0] = jnp.floor(partial * FIXED + 0.5).astype(i32).astype(i16)


def cosines(slots, a, a_at, b, width):
    pairs = slots.shape[0]
    spec = pltpu.PrefetchScalarGridSpec(
        num_scalar_prefetch=2,
        grid=(pairs,),
        in_specs=[
            pl.BlockSpec((1, width, HALF), lambda q, s, r: (s[q], 0, a_at)),
            pl.BlockSpec((1, width, BS), lambda q, s, r: (r[q], 0, 0)),
        ],
        out_specs=pl.BlockSpec((1, HALF, BS), lambda q, s, r: (q, 0, 0)),
    )
    shape = jax.ShapeDtypeStruct((pairs, HALF, BS), i16)
    flops = 2 * pairs * HALF * BS * width
    moved = pairs * (width * (HALF + BS) + HALF * BS) * 2
    return call(cosine_kernel, shape, spec, flops, moved, (slots[:, 0], slots[:, 1], a, b))


def both_cores_kernel(x_ref, *refs):
    ins, outs = refs[:8], refs[8:]
    for d in range(4):
        total = ins[d][...].astype(i32) + ins[4 + d][...].astype(i32)
        outs[d][...] = total.astype(i16)


def both_cores(chip, own, other):
    each = own.shape[0] // 4
    block = (1, HALF, BS)

    def at(d):
        return pl.BlockSpec(block, lambda k, x: (lax.rem(x[0] + d, 4) * each + k, 0, 0))

    spec = pltpu.PrefetchScalarGridSpec(
        num_scalar_prefetch=1,
        grid=(each,),
        in_specs=[at(d) for d in range(4)] * 2,
        out_specs=[pl.BlockSpec(block, lambda k, x: (k, 0, 0))] * 4,
    )
    shape = [jax.ShapeDtypeStruct((each, HALF, BS), i16)] * 4
    size = own.size
    return call(
        both_cores_kernel, shape, spec, size, 6 * size, (chip, *([own] * 4), *([other] * 4))
    )


def affinity_kernel(a_ref, b_ref, c_ref, d_ref, out_ref, turned_ref):
    total = a_ref[0].astype(i32) + b_ref[0].astype(i32)
    total = total + c_ref[0].astype(i32) + d_ref[0].astype(i32)
    value = jnp.exp(total.astype(f32) * (1.0 / (FIXED * smoothing_regularizer)))
    out_ref[0] = value
    turned_ref[0] = value.T


def affinity(parts):
    each = parts[0].shape[0]
    spec = pl.GridSpec(
        grid=(each,),
        in_specs=[pl.BlockSpec((1, HALF, BS), lambda k: (k, 0, 0))] * 4,
        out_specs=[
            pl.BlockSpec((1, HALF, BS), lambda k: (k, 0, 0)),
            pl.BlockSpec((1, BS, HALF), lambda k: (k, 0, 0)),
        ],
    )
    shape = [
        jax.ShapeDtypeStruct((each, HALF, BS), f32),
        jax.ShapeDtypeStruct((each, BS, HALF), f32),
    ]
    size = each * HALF * BS
    return call(affinity_kernel, shape, spec, 8 * size, 16 * size, tuple(parts))


def emit_rows(rows, fine, out_ref, scratch):
    pad = scratch.shape[0] - len(rows)
    tile = jnp.concatenate(rows + [jnp.zeros((pad, LANES), f32)], axis=0)
    high = tile.astype(bf16)
    if fine:
        low = (tile - high.astype(f32)).astype(bf16)
        high = jnp.concatenate([high, low], axis=0)
    out_ref[...] = jnp.broadcast_to(high[None], out_ref.shape)


def times_rows(mats, scale):
    turned = None if scale is None else scale.T
    rows = []
    for k in range(mats[0].shape[0]):
        if len(mats) == 2 and mats[0].shape[1] == HALF:
            total = None
            for j in range(TILES):
                part = mats[j // 2][k, (j % 2) * LANES : (j % 2 + 1) * LANES, :]
                if turned is not None:
                    part = part * turned[:, TILES * k + j : TILES * k + j + 1]
                part = jnp.sum(part, axis=0, keepdims=True)
                total = part if total is None else total + part
            rows += [total[:, j * LANES : (j + 1) * LANES] for j in range(TILES)]
        else:
            for m in mats:
                total = None
                for j in range(TILES):
                    part = m[k, j * LANES : (j + 1) * LANES, :]
                    if turned is not None:
                        part = part * turned[:, TILES * k + j : TILES * k + j + 1]
                    part = jnp.sum(part, axis=0, keepdims=True)
                    total = part if total is None else total + part
                rows += [total[:, j * LANES : (j + 1) * LANES] for j in range(TILES // 2)]
    return rows


def start_kernel(first_ref, second_ref, out_ref, scratch):
    emit_rows(times_rows((first_ref, second_ref), None), False, out_ref, scratch)


def totals_of(hot, got_ref):
    got = got_ref[...].reshape(-1, LANES)
    return jnp.dot(hot, got, preferred_element_type=f32)


def step_kernel(fine, got_ref, hot_ref, first_ref, second_ref, out_ref, scratch):
    scale = 1.0 / (1.0 + totals_of(hot_ref[...], got_ref))
    padded = jnp.concatenate([scale, jnp.zeros((LANES - scale.shape[0], LANES), f32)], axis=0)
    emit_rows(times_rows((first_ref, second_ref), padded), fine, out_ref, scratch)


def log_kernel(got_ref, hot_ref, log_ref):
    log_ref[...] = jnp.log(1.0 / (1.0 + totals_of(hot_ref[...], got_ref)))


def on_chip(kernel, out_shape, flops, args, scratch=()):
    return pl.pallas_call(
        kernel,
        out_shape=out_shape,
        in_specs=[pl.BlockSpec(memory_space=pltpu.VMEM)] * len(args),
        out_specs=pl.BlockSpec(memory_space=pltpu.VMEM),
        scratch_shapes=list(scratch),
        compiler_params=pltpu.CompilerParams(vmem_limit_bytes=24 * 2**20),
        cost_estimate=pl.CostEstimate(flops=flops, bytes_accessed=flops, transcendentals=0),
    )(*args)


ROWS = 16


def step(got, hot, mats, fine, devices):
    out = jax.ShapeDtypeStruct((devices, 2 * ROWS if fine else ROWS, LANES), bf16)
    scratch = [pltpu.VMEM((ROWS, LANES), f32)]
    flops = 4 * mats[0].size
    if got is None:
        return on_chip(start_kernel, out, flops, tuple(mats), scratch)
    return on_chip(
        functools.partial(step_kernel, fine), out, flops, (got, hot, *mats), scratch
    )


def exchanged(x):
    return lax.all_to_all(x, ALL, 0, 0, tiled=True)


def hot_rows(wanted, present, fine):
    devices, pairs = present.shape
    col = jnp.full((devices, ROWS // TILES), -1, i32).at[:, :pairs].set(present)
    col_id = jnp.broadcast_to(col[:, :, None], (devices, ROWS // TILES, TILES))
    col_tile = jnp.broadcast_to(jnp.arange(TILES)[None, None, :], col_id.shape)
    if fine:
        col_id = jnp.concatenate([col_id, col_id], axis=1)
        col_tile = jnp.concatenate([col_tile, col_tile], axis=1)
    row_id = jnp.repeat(wanted, TILES)
    row_tile = jnp.tile(jnp.arange(TILES), wanted.shape[0])
    same = (row_id[:, None] == col_id.reshape(-1)[None, :]) & (
        row_tile[:, None] == col_tile.reshape(-1)[None, :]
    )
    return same.astype(bf16)


def per_device(initial_dictionary_matrix, decoder_two, route_one, route_two, candidate_pair_slots):
    column = lax.axis_index(BA)
    chip = lax.axis_index("aa_0")
    core = lax.axis_index("aa_1")
    owners = lax.axis_size(BA)
    depth = lax.axis_size(AA)
    devices = owners * depth
    blocks_dev = initial_dictionary_matrix.shape[0] // BS
    width = initial_dictionary_matrix.shape[1]

    one_t, two_t = initial_dictionary_matrix.T, decoder_two.T
    sums = jnp.concatenate(
        [jnp.sum(jnp.square(t.astype(f32)), axis=0) for t in (one_t, two_t)]
    )
    sums = sums.reshape(8, -1)
    sums = lax.all_to_all(
        jnp.broadcast_to(sums[None], (depth, *sums.shape)), AA, 0, 0, tiled=True
    ).sum(axis=0)
    inverse = lax.rsqrt(sums + norm_floor).reshape(2, 1, -1)

    my_one = lax.dynamic_index_in_dim(route_one, column, 0, False)
    my_two = lax.dynamic_index_in_dim(route_two, column, 0, False)
    slots = candidate_pair_slots[0]
    pairs = slots.shape[0]
    ids = jnp.zeros((IDS, HALF), bf16).at[:2, :pairs].set(slots.T.astype(bf16))
    first = pack_first(my_one, my_two, one_t, two_t, inverse[0], inverse[1])
    second = pack_second(my_one, one_t, inverse[0], ids)
    first = lax.all_to_all(first, BA, 0, 0, tiled=True)

    mine = pairs // 2
    own_slots = lax.dynamic_slice_in_dim(slots, core * mine, mine, 0)
    other_slots = lax.dynamic_slice_in_dim(slots, (1 - core) * mine, mine, 0)
    swap = [(0, 1), (1, 0)]
    chip_list = chip.reshape(1).astype(i32)

    def summed(a, a_at):
        other = cosines(other_slots, a, a_at, first, width)
        other = lax.ppermute(other, "aa_1", swap)
        own = cosines(own_slots, a, a_at, first, width)
        parts = both_cores(chip_list, own, other)
        return [parts[0]] + [
            lax.ppermute(parts[d], "aa_0", [(x, (x + d) % 4) for x in range(4)])
            for d in range(1, 4)
        ]

    upper = summed(first, 2)
    second = lax.all_to_all(second, BA, 0, 0, tiled=True)
    lower = summed(second, 0)
    k_upper, t_upper = affinity(upper)
    k_lower, t_lower = affinity(lower)

    every = second[:, width : width + 2, :pairs].astype(i32)
    owner_ids = jnp.arange(owners)[:, None]
    s_all, r_all = every[:, 0], every[:, 1]
    row_all = s_all * blocks_dev + route_one[s_all, owner_ids]
    col_all = r_all * blocks_dev + route_two[r_all, owner_ids]
    each = pairs // depth

    def by_device(x):
        x = x.reshape(owners, 2, 4, each)
        return x.transpose(2, 1, 0, 3).reshape(devices, each)

    row_dev, col_dev = by_device(row_all), by_device(col_all)
    me = (chip * 2 + core) * owners + column
    my_rows = lax.dynamic_index_in_dim(row_dev, me, 0, False)
    my_cols = lax.dynamic_index_in_dim(col_dev, me, 0, False)
    pad = jnp.full((ROWS // TILES - each,), -2, i32)
    my_rows = jnp.concatenate([my_rows, pad])
    my_cols = jnp.concatenate([my_cols, pad])
    own_blocks = column * blocks_dev + jnp.arange(blocks_dev)
    row_hot = hot_rows(my_rows, row_dev, False)
    col_hot = hot_rows(my_cols, col_dev, False)
    row_hot_fine = hot_rows(my_rows, row_dev, True)
    row_hot_own = hot_rows(own_blocks, row_dev, True)
    col_hot_own = hot_rows(own_blocks, col_dev, True)

    by_row, by_col = (t_upper, t_lower), (k_upper, k_lower)
    got = exchanged(step(None, None, by_row, False, devices))
    for sweep in range(SWEEPS - 1):
        got = exchanged(step(got, row_hot, by_col, False, devices))
        got = exchanged(step(got, col_hot, by_row, sweep == SWEEPS - 2, devices))
    logs = jax.ShapeDtypeStruct((blocks_dev * TILES, LANES), f32)
    last = exchanged(step(got, row_hot_fine, by_col, True, devices))
    row_log = on_chip(log_kernel, logs, 2**20, (got, row_hot_own))
    col_log = on_chip(log_kernel, logs, 2**20, (last, col_hot_own))
    return row_log.reshape(-1), col_log.reshape(-1)


def solution(mesh):
    torus = Mesh(mesh.devices.reshape(4, 2, 4, 4), ("aa_0", "aa_1", "ba_0", "ba_1"))
    in_specs = (P(BA, AA), P(BA, AA), P(), P(), P(BA, None, None))
    out_specs = (P(BA), P(BA))
    return jax.shard_map(
        per_device, mesh=torus, in_specs=in_specs, out_specs=out_specs, check_vma=False
    )
```

```python
import jax
import jax.numpy as jnp
from jax import lax
from jax.experimental import pallas as pl
from jax.experimental.pallas import tpu as pltpu
from jax.sharding import Mesh
from jax.sharding import PartitionSpec as P

BS = 512
SWEEPS = 4
BA = ("ba_0", "ba_1")
AA = ("aa_0", "aa_1")
ALL = AA + BA
LANES = 128
TILES = BS // LANES
HALF = BS // 2
FIXED = 32000.0
IDS = 16

smoothing_regularizer = 0.02
norm_floor = 1e-06

f32, bf16, i16, i32 = jnp.float32, jnp.bfloat16, jnp.int16, jnp.int32


def call(kernel, out_shape, grid_spec, flops, bytes_accessed, args):
    return pl.pallas_call(
        kernel,
        out_shape=out_shape,
        grid_spec=grid_spec,
        compiler_params=pltpu.CompilerParams(vmem_limit_bytes=8 * 2**20),
        cost_estimate=pl.CostEstimate(
            flops=flops, bytes_accessed=bytes_accessed, transcendentals=0
        ),
    )(*args)


def pack_kernel(one_ref, two_ref, a_ref, b_ref, inv_a_ref, inv_b_ref, ids_ref, first_ref, second_ref):
    width = a_ref.shape[0]
    unit_a = (a_ref[...].astype(f32) * inv_a_ref[...]).astype(bf16)
    first_ref[0, :, :BS] = (b_ref[...].astype(f32) * inv_b_ref[...]).astype(bf16)
    first_ref[0, :, BS:] = unit_a[:, :HALF]
    second_ref[0, :width, :] = unit_a[:, HALF:]
    second_ref[0, width:, :] = ids_ref[...]


def pack(one, two, a, b, inv_a, inv_b, ids):
    width, owners = a.shape[0], one.shape[0]
    spec = pltpu.PrefetchScalarGridSpec(
        num_scalar_prefetch=2,
        grid=(owners,),
        in_specs=[
            pl.BlockSpec((width, BS), lambda o, r1, r2: (0, r1[o])),
            pl.BlockSpec((width, BS), lambda o, r1, r2: (0, r2[o])),
            pl.BlockSpec((1, BS), lambda o, r1, r2: (0, r1[o])),
            pl.BlockSpec((1, BS), lambda o, r1, r2: (0, r2[o])),
            pl.BlockSpec((IDS, HALF), lambda o, r1, r2: (0, 0)),
        ],
        out_specs=[
            pl.BlockSpec((1, width, BS + HALF), lambda o, r1, r2: (o, 0, 0)),
            pl.BlockSpec((1, width + IDS, HALF), lambda o, r1, r2: (o, 0, 0)),
        ],
    )
    shape = [
        jax.ShapeDtypeStruct((owners, width, BS + HALF), bf16),
        jax.ShapeDtypeStruct((owners, width + IDS, HALF), bf16),
    ]
    size = owners * width * 2 * BS
    return call(pack_kernel, shape, spec, 2 * size, 4 * size, (one, two, a, b, inv_a, inv_b, ids))


def cosine_kernel(s_ref, r_ref, a_ref, b_ref, out_ref):
    partial = lax.dot_general(
        a_ref[0], b_ref[0], (((0,), (0,)), ((), ())), preferred_element_type=f32
    )
    out_ref[0] = jnp.floor(partial * FIXED + 0.5).astype(i32).astype(i16)


def cosines(sources, a, a_at, b, width):
    pairs = sources[0].shape[0]
    spec = pltpu.PrefetchScalarGridSpec(
        num_scalar_prefetch=2,
        grid=(pairs,),
        in_specs=[
            pl.BlockSpec((1, width, HALF), lambda q, s, r: (s[q], 0, a_at)),
            pl.BlockSpec((1, width, BS), lambda q, s, r: (r[q], 0, 0)),
        ],
        out_specs=pl.BlockSpec((1, HALF, BS), lambda q, s, r: (q, 0, 0)),
    )
    shape = jax.ShapeDtypeStruct((pairs, HALF, BS), i16)
    flops = 2 * pairs * HALF * BS * width
    moved = pairs * (width * (HALF + BS) + HALF * BS) * 2
    return call(cosine_kernel, shape, spec, flops, moved, (*sources, a, b))


def both_cores_kernel(x_ref, *refs):
    ins, outs = refs[:8], refs[8:]
    for d in range(4):
        total = ins[d][...].astype(i32) + ins[4 + d][...].astype(i32)
        outs[d][...] = total.astype(i16)


def both_cores(chip, own, other):
    each = own.shape[0] // 4
    block = (1, HALF, BS)

    def at(d):
        return pl.BlockSpec(block, lambda k, x: (lax.rem(x[0] + d, 4) * each + k, 0, 0))

    spec = pltpu.PrefetchScalarGridSpec(
        num_scalar_prefetch=1,
        grid=(each,),
        in_specs=[at(d) for d in range(4)] * 2,
        out_specs=[pl.BlockSpec(block, lambda k, x: (k, 0, 0))] * 4,
    )
    shape = [jax.ShapeDtypeStruct((each, HALF, BS), i16)] * 4
    size = own.size
    return call(
        both_cores_kernel, shape, spec, size, 6 * size, (chip, *([own] * 4), *([other] * 4))
    )


def affinity_kernel(a_ref, b_ref, c_ref, d_ref, out_ref, turned_ref):
    total = a_ref[0].astype(i32) + b_ref[0].astype(i32)
    total = total + c_ref[0].astype(i32) + d_ref[0].astype(i32)
    value = jnp.exp(total.astype(f32) * (1.0 / (FIXED * smoothing_regularizer)))
    out_ref[0] = value
    turned_ref[0] = value.T


def affinity(parts):
    each = parts[0].shape[0]
    spec = pl.GridSpec(
        grid=(each,),
        in_specs=[pl.BlockSpec((1, HALF, BS), lambda k: (k, 0, 0))] * 4,
        out_specs=[
            pl.BlockSpec((1, HALF, BS), lambda k: (k, 0, 0)),
            pl.BlockSpec((1, BS, HALF), lambda k: (k, 0, 0)),
        ],
    )
    shape = [
        jax.ShapeDtypeStruct((each, HALF, BS), f32),
        jax.ShapeDtypeStruct((each, BS, HALF), f32),
    ]
    size = each * HALF * BS
    return call(affinity_kernel, shape, spec, 8 * size, 16 * size, tuple(parts))


def emit_rows(rows, out_ref):
    high = [r.astype(bf16).astype(f32) for r in rows]
    low = [r - h for r, h in zip(rows, high)]
    tile = jnp.concatenate(high + low, axis=0).astype(bf16)
    out_ref[...] = jnp.broadcast_to(tile[None], out_ref.shape)


def times_rows(mats, scale):
    turned = None if scale is None else scale.T
    rows = []
    for k in range(mats[0].shape[0]):
        if len(mats) == 2 and mats[0].shape[1] == HALF:
            total = None
            for j in range(TILES):
                part = mats[j // 2][k, (j % 2) * LANES : (j % 2 + 1) * LANES, :]
                if turned is not None:
                    part = part * turned[:, TILES * k + j : TILES * k + j + 1]
                part = jnp.sum(part, axis=0, keepdims=True)
                total = part if total is None else total + part
            rows += [total[:, j * LANES : (j + 1) * LANES] for j in range(TILES)]
        else:
            for m in mats:
                total = None
                for j in range(TILES):
                    part = m[k, j * LANES : (j + 1) * LANES, :]
                    if turned is not None:
                        part = part * turned[:, TILES * k + j : TILES * k + j + 1]
                    part = jnp.sum(part, axis=0, keepdims=True)
                    total = part if total is None else total + part
                rows += [total[:, j * LANES : (j + 1) * LANES] for j in range(TILES // 2)]
    return rows


def start_kernel(first_ref, second_ref, out_ref):
    emit_rows(times_rows((first_ref, second_ref), None), out_ref)


def totals_of(hot, got_ref):
    got = got_ref[...].reshape(-1, LANES)
    return jnp.dot(hot, got, preferred_element_type=f32)


def step_kernel(got_ref, hot_ref, first_ref, second_ref, out_ref):
    scale = 1.0 / (1.0 + totals_of(hot_ref[...], got_ref))
    padded = jnp.concatenate([scale, jnp.zeros((LANES - scale.shape[0], LANES), f32)], axis=0)
    emit_rows(times_rows((first_ref, second_ref), padded), out_ref)


def log_kernel(got_ref, hot_ref, log_ref):
    log_ref[...] = jnp.log(1.0 / (1.0 + totals_of(hot_ref[...], got_ref)))


def on_chip(kernel, out_shape, flops, args):
    return pl.pallas_call(
        kernel,
        out_shape=out_shape,
        in_specs=[pl.BlockSpec(memory_space=pltpu.VMEM)] * len(args),
        out_specs=pl.BlockSpec(memory_space=pltpu.VMEM),
        compiler_params=pltpu.CompilerParams(vmem_limit_bytes=8 * 2**20),
        cost_estimate=pl.CostEstimate(flops=flops, bytes_accessed=flops, transcendentals=0),
    )(*args)


def step(got, hot, mats, devices):
    rows = 2 * TILES * mats[0].shape[0]
    out = jax.ShapeDtypeStruct((devices, rows, LANES), bf16)
    flops = 4 * mats[0].size
    if got is None:
        return on_chip(start_kernel, out, flops, tuple(mats))
    return on_chip(step_kernel, out, flops, (got, hot, *mats))


def exchanged(x):
    return lax.all_to_all(x, ALL, 0, 0, tiled=True)


def hot_rows(wanted, present):
    devices, pairs = present.shape
    shape = (devices, 2, pairs, TILES)
    col_id = jnp.broadcast_to(present[:, None, :, None], shape).reshape(1, -1)
    col_tile = lax.broadcasted_iota(i32, shape, 3).reshape(1, -1)
    row_id = jnp.repeat(wanted, TILES)[:, None]
    row_tile = jnp.tile(jnp.arange(TILES), wanted.shape[0])[:, None]
    return ((row_id == col_id) & (row_tile == col_tile)).astype(bf16)


tied = lax.optimization_barrier


def per_device(initial_dictionary_matrix, decoder_two, route_one, route_two, candidate_pair_slots):
    column = lax.axis_index(BA)
    chip = lax.axis_index("aa_0")
    core = lax.axis_index("aa_1")
    owners = lax.axis_size(BA)
    depth = lax.axis_size(AA)
    devices = owners * depth
    blocks_dev = initial_dictionary_matrix.shape[0] // BS
    width = initial_dictionary_matrix.shape[1]

    one_t, two_t = initial_dictionary_matrix.T, decoder_two.T
    sums = jnp.concatenate(
        [jnp.sum(jnp.square(t.astype(f32)), axis=0) for t in (one_t, two_t)]
    )
    sums = sums.reshape(8, -1)
    my_one = lax.dynamic_index_in_dim(route_one, column, 0, False)
    my_two = lax.dynamic_index_in_dim(route_two, column, 0, False)
    slots = candidate_pair_slots[0]
    pairs = slots.shape[0]
    ids = jnp.zeros((IDS, HALF), bf16).at[:2, :pairs].set(slots.T.astype(bf16))
    mine = pairs // 2

    def of_core(which):
        return [lax.dynamic_slice_in_dim(slots[:, i], which * mine, mine, 0) for i in range(2)]

    own_slots, other_slots = of_core(core), of_core(1 - core)
    chip_list = chip.reshape(1).astype(i32)
    small = (my_one, my_two, ids, own_slots, other_slots, chip_list)
    sums, small = tied((sums, small))
    my_one, my_two, ids, own_slots, other_slots, chip_list = small
    sums = lax.all_to_all(
        jnp.broadcast_to(sums[None], (depth, *sums.shape)), AA, 0, 0, tiled=True
    ).sum(axis=0)
    inverse = lax.rsqrt(sums + norm_floor).reshape(2, 1, -1)

    first, second = pack(my_one, my_two, one_t, two_t, inverse[0], inverse[1], ids)
    first, second = tied((first, second))
    first = lax.all_to_all(first, BA, 0, 0, tiled=True)
    first, second = tied((first, second))
    swap = [(0, 1), (1, 0)]

    def by_chip(a, a_at):
        other = cosines(other_slots, a, a_at, first, width)
        other = lax.ppermute(other, "aa_1", swap)
        own = cosines(own_slots, a, a_at, first, width)
        return both_cores(chip_list, own, other)

    def to_chips(parts):
        return [parts[0]] + [
            lax.ppermute(parts[d], "aa_0", [(x, (x + d) % 4) for x in range(4)])
            for d in range(1, 4)
        ]

    parts = by_chip(first, 2)
    parts, second = tied((parts, second))
    upper = to_chips(parts)
    second = lax.all_to_all(second, BA, 0, 0, tiled=True)
    parts, second = tied((by_chip(second, 0), second))
    lower = to_chips(parts)
    k_upper, t_upper = affinity(upper)
    k_lower, t_lower = affinity(lower)

    def masks():
        every = second[:, width : width + 2, :pairs].astype(i32)
        s_all, r_all = every[:, 0], every[:, 1]

        def block_of(source, route):
            chosen = source[:, :, None] == jnp.arange(owners)[None, None, :]
            return source * blocks_dev + jnp.sum(jnp.where(chosen, route.T[:, None, :], 0), axis=2)

        each = pairs // depth

        def by_device(x):
            x = x.reshape(owners, 2, 4, each)
            return x.transpose(2, 1, 0, 3).reshape(devices, each)

        row_dev, col_dev = by_device(block_of(s_all, route_one)), by_device(block_of(r_all, route_two))
        me = (chip * 2 + core) * owners + column
        pad = jnp.full((4 - each,), -2, i32)
        my_rows = jnp.concatenate([lax.dynamic_index_in_dim(row_dev, me, 0, False), pad])
        my_cols = jnp.concatenate([lax.dynamic_index_in_dim(col_dev, me, 0, False), pad])
        own_blocks = column * blocks_dev + jnp.arange(blocks_dev)
        return [
            hot_rows(my_rows, row_dev),
            hot_rows(my_cols, col_dev),
            hot_rows(own_blocks, row_dev),
            hot_rows(own_blocks, col_dev),
        ]

    hot = masks()

    mats, hot = tied(((k_upper, k_lower, t_upper, t_lower), hot))
    by_row, by_col = mats[2:], mats[:2]
    got = exchanged(step(None, None, by_row, devices))
    for _ in range(SWEEPS - 1):
        got = exchanged(step(got, hot[0], by_col, devices))
        got = exchanged(step(got, hot[1], by_row, devices))
    last = exchanged(step(got, hot[0], by_col, devices))
    got, last = tied((got, last))
    logs = jax.ShapeDtypeStruct((blocks_dev * TILES, LANES), f32)
    row_log = on_chip(log_kernel, logs, 2**20, (got, hot[2]))
    col_log = on_chip(log_kernel, logs, 2**20, (last, hot[3]))
    return row_log.reshape(-1), col_log.reshape(-1)


def solution(mesh):
    torus = Mesh(mesh.devices.reshape(4, 2, 4, 4), ("aa_0", "aa_1", "ba_0", "ba_1"))
    in_specs = (P(BA, AA), P(BA, AA), P(), P(), P(BA, None, None))
    out_specs = (P(BA), P(BA))
    return jax.shard_map(
        per_device, mesh=torus, in_specs=in_specs, out_specs=out_specs, check_vma=False
    )
```

```python
import jax
import jax.numpy as jnp
from jax import lax
from jax.experimental import pallas as pl
from jax.experimental.pallas import tpu as pltpu
from jax.sharding import Mesh
from jax.sharding import PartitionSpec as P

BS = 512
SWEEPS = 4
BA = ("ba_0", "ba_1")
AA = ("aa_0", "aa_1")
ALL = AA + BA
LANES = 128
TILES = BS // LANES
UPPER = 3 * LANES
FIXED = 32000.0
IDS = 16


smoothing_regularizer = 0.02
norm_floor = 1e-06

f32, bf16, i16, i32 = jnp.float32, jnp.bfloat16, jnp.int16, jnp.int32


def call(kernel, out_shape, grid_spec, flops, bytes_accessed, args, mebibytes=8):
    return pl.pallas_call(
        kernel,
        out_shape=out_shape,
        grid_spec=grid_spec,
        compiler_params=pltpu.CompilerParams(vmem_limit_bytes=mebibytes * 2**20),
        cost_estimate=pl.CostEstimate(
            flops=flops, bytes_accessed=bytes_accessed, transcendentals=0
        ),
    )(*args)


def squares_kernel(one_ref, two_ref, sums_ref):
    for i, ref in enumerate((one_ref, two_ref)):
        total = jnp.sum(jnp.square(ref[...].astype(f32)), axis=0, keepdims=True)
        sums_ref[:, i : i + 1, :] = jnp.broadcast_to(total[None], (sums_ref.shape[0], 1, BS))


def squares(one, two, depth):
    width, rows = one.shape
    block = pl.BlockSpec((width, BS), lambda k: (0, k))
    spec = pl.GridSpec(
        grid=(rows // BS,),
        in_specs=[block, block],
        out_specs=pl.BlockSpec((depth, 2, BS), lambda k: (0, 0, k)),
    )
    shape = jax.ShapeDtypeStruct((depth, 2, rows), f32)
    return call(squares_kernel, shape, spec, 4 * one.size, 8 * one.size, (one, two), 60)


def pack_kernel(
    me_ref, one_ref, two_ref, a_ref, b_ref, inv_a_ref, inv_b_ref, slots_ref, first_ref, second_ref
):
    width, pairs = a_ref.shape[0], slots_ref.shape[1]
    unit_a = (a_ref[...].astype(f32) * inv_a_ref[0:1, :]).astype(bf16)
    first_ref[0, :, :BS] = (b_ref[...].astype(f32) * inv_b_ref[1:2, :]).astype(bf16)
    first_ref[0, :, BS:] = unit_a[:, :UPPER]
    second_ref[0, :width, :] = unit_a[:, UPPER:]
    second_ref[0, width:, :] = jnp.zeros((IDS, LANES), bf16)
    second_ref[0, width : width + 2, :pairs] = slots_ref[...].astype(f32).astype(bf16)


def pack(me, one, two, a, b, inverse, slots):
    width, owners = a.shape[0], one.shape[0]
    spec = pltpu.PrefetchScalarGridSpec(
        num_scalar_prefetch=3,
        grid=(owners,),
        in_specs=[
            pl.BlockSpec((width, BS), lambda o, me, r1, r2: (0, r1[me[0], o])),
            pl.BlockSpec((width, BS), lambda o, me, r1, r2: (0, r2[me[0], o])),
            pl.BlockSpec((2, BS), lambda o, me, r1, r2: (0, r1[me[0], o])),
            pl.BlockSpec((2, BS), lambda o, me, r1, r2: (0, r2[me[0], o])),
            pl.BlockSpec(slots.shape, lambda o, me, r1, r2: (0, 0)),
        ],
        out_specs=[
            pl.BlockSpec((1, width, BS + UPPER), lambda o, me, r1, r2: (o, 0, 0)),
            pl.BlockSpec((1, width + IDS, LANES), lambda o, me, r1, r2: (o, 0, 0)),
        ],
    )
    shape = [
        jax.ShapeDtypeStruct((owners, width, BS + UPPER), bf16),
        jax.ShapeDtypeStruct((owners, width + IDS, LANES), bf16),
    ]
    size = owners * width * 2 * BS
    args = (me, one, two, a, b, inverse, inverse, slots)
    return call(pack_kernel, shape, spec, 2 * size, 4 * size, args)


def cosine_kernel(core_ref, slots_ref, *refs):
    out_ref, b_ref, tiles = refs[-1], refs[-2], refs[:-2]
    for t, a_ref in enumerate(tiles):
        partial = lax.dot_general(
            a_ref[0], b_ref[0], (((0,), (0,)), ((), ())), preferred_element_type=f32
        )
        fixed = jnp.floor(partial * FIXED + 0.5).astype(i32).astype(i16)
        out_ref[0, t * LANES : (t + 1) * LANES, :] = fixed


def cosines(core, slots, a, tiles, b, width):
    pairs = slots.shape[1] // 2

    def tile(t):
        return pl.BlockSpec((1, width, LANES), lambda q, c, s: (s[0, c[0] * pairs + q], 0, t))

    rows = LANES * len(tiles)
    spec = pltpu.PrefetchScalarGridSpec(
        num_scalar_prefetch=2,
        grid=(pairs,),
        in_specs=[tile(t) for t in tiles]
        + [pl.BlockSpec((1, width, BS), lambda q, c, s: (s[1, c[0] * pairs + q], 0, 0))],
        out_specs=pl.BlockSpec((1, rows, BS), lambda q, c, s: (q, 0, 0)),
    )
    shape = jax.ShapeDtypeStruct((pairs, rows, BS), i16)
    flops = 2 * pairs * rows * BS * width
    moved = pairs * (width * (rows + BS) + rows * BS) * 2
    return call(cosine_kernel, shape, spec, flops, moved, (core, slots, *([a] * len(tiles)), b))


def both_cores_kernel(x_ref, *refs):
    ins, outs = refs[:8], refs[8:]
    for d in range(4):
        total = ins[d][...].astype(i32) + ins[4 + d][...].astype(i32)
        outs[d][...] = total.astype(i16)


def both_cores(chip, own, other):
    each = own.shape[0] // 4
    block = (1, *own.shape[1:])

    def at(d):
        return pl.BlockSpec(block, lambda k, x: (lax.rem(x[0] + d, 4) * each + k, 0, 0))

    spec = pltpu.PrefetchScalarGridSpec(
        num_scalar_prefetch=1,
        grid=(each,),
        in_specs=[at(d) for d in range(4)] * 2,
        out_specs=[pl.BlockSpec(block, lambda k, x: (k, 0, 0))] * 4,
    )
    shape = [jax.ShapeDtypeStruct((each, *own.shape[1:]), i16)] * 4
    size = own.size
    return call(
        both_cores_kernel, shape, spec, size, 6 * size, (chip, *([own] * 4), *([other] * 4))
    )


def affinity_kernel(a_ref, b_ref, c_ref, d_ref, out_ref, turned_ref):
    total = a_ref[0].astype(i32) + b_ref[0].astype(i32)
    total = total + c_ref[0].astype(i32) + d_ref[0].astype(i32)
    value = jnp.exp(total.astype(f32) * (1.0 / (FIXED * smoothing_regularizer)))
    out_ref[0] = value
    turned_ref[0] = value.T


def affinity(parts):
    each, rows, cols = parts[0].shape
    spec = pl.GridSpec(
        grid=(each,),
        in_specs=[pl.BlockSpec((1, rows, cols), lambda k: (k, 0, 0))] * 4,
        out_specs=[
            pl.BlockSpec((1, rows, cols), lambda k: (k, 0, 0)),
            pl.BlockSpec((1, cols, rows), lambda k: (k, 0, 0)),
        ],
    )
    shape = [
        jax.ShapeDtypeStruct((each, rows, cols), f32),
        jax.ShapeDtypeStruct((each, cols, rows), f32),
    ]
    size = each * rows * cols
    return call(affinity_kernel, shape, spec, 8 * size, 16 * size, tuple(parts))


def emit_rows(rows, out_ref):
    high = [r.astype(bf16).astype(f32) for r in rows]
    low = [r - h for r, h in zip(rows, high)]
    tile = jnp.concatenate(high + low, axis=0).astype(bf16)
    out_ref[...] = jnp.broadcast_to(tile[None], out_ref.shape)


def times_rows(mats, scale):
    turned = None if scale is None else scale.T

    def tile(m, at, k, j):
        part = m[k, at * LANES : (at + 1) * LANES, :]
        if turned is not None:
            part = part * turned[:, TILES * k + j : TILES * k + j + 1]
        return jnp.sum(part, axis=0, keepdims=True)

    rows = []
    for k in range(mats[0].shape[0]):
        if mats[0].shape[1] == BS:
            groups = [[tile(m, j, k, j) for j in range(TILES)] for m in mats]
        else:
            places = [(m, at) for m in mats for at in range(m.shape[1] // LANES)]
            groups = [[tile(m, at, k, j) for j, (m, at) in enumerate(places)]]
        for g in groups:
            total = (g[0] + g[1]) + (g[2] + g[3])
            rows += [total[:, t : t + LANES] for t in range(0, total.shape[1], LANES)]
    return rows


def start_kernel(first_ref, second_ref, out_ref):
    emit_rows(times_rows((first_ref, second_ref), None), out_ref)


def totals_of(hot, got_ref):
    got = got_ref[...].reshape(-1, LANES)
    return jnp.dot(hot, got, preferred_element_type=f32)


def step_kernel(got_ref, hot_ref, first_ref, second_ref, out_ref):
    scale = 1.0 / (1.0 + totals_of(hot_ref[...], got_ref))
    padded = jnp.concatenate([scale, jnp.zeros((LANES - scale.shape[0], LANES), f32)], axis=0)
    emit_rows(times_rows((first_ref, second_ref), padded), out_ref)


def log_kernel(row_got_ref, row_hot_ref, col_got_ref, col_hot_ref, row_log_ref, col_log_ref):
    row_log_ref[...] = jnp.log(1.0 / (1.0 + totals_of(row_hot_ref[...], row_got_ref)))
    col_log_ref[...] = jnp.log(1.0 / (1.0 + totals_of(col_hot_ref[...], col_got_ref)))


def on_chip(kernel, out_shape, flops, args):
    return pl.pallas_call(
        kernel,
        out_shape=out_shape,
        in_specs=[pl.BlockSpec(memory_space=pltpu.VMEM)] * len(args),
        out_specs=jax.tree.map(lambda _: pl.BlockSpec(memory_space=pltpu.VMEM), out_shape),
        compiler_params=pltpu.CompilerParams(vmem_limit_bytes=8 * 2**20),
        cost_estimate=pl.CostEstimate(flops=flops, bytes_accessed=flops, transcendentals=0),
    )(*args)


def step(got, hot, mats, devices):
    rows = 2 * TILES * mats[0].shape[0]
    out = jax.ShapeDtypeStruct((devices, rows, LANES), bf16)
    flops = 4 * mats[0].size
    if got is None:
        return on_chip(start_kernel, out, flops, tuple(mats))
    return on_chip(step_kernel, out, flops, (got, hot, *mats))


def exchanged(x):
    return lax.all_to_all(x, ALL, 0, 0, tiled=True)


def hot_rows(wanted, present):
    devices, pairs = present.shape
    shape = (devices, 2, pairs, TILES)
    col_id = jnp.broadcast_to(present[:, None, :, None], shape).reshape(1, -1)
    col_tile = lax.broadcasted_iota(i32, shape, 3).reshape(1, -1)
    row_id = jnp.repeat(wanted, TILES)[:, None]
    row_tile = jnp.tile(jnp.arange(TILES), wanted.shape[0])[:, None]
    return ((row_id == col_id) & (row_tile == col_tile)).astype(bf16)


tied = lax.optimization_barrier


def per_device(initial_dictionary_matrix, decoder_two, route_one, route_two, candidate_pair_slots):
    column = lax.axis_index(BA)
    chip = lax.axis_index("aa_0")
    core = lax.axis_index("aa_1")
    owners = lax.axis_size(BA)
    depth = lax.axis_size(AA)
    devices = owners * depth
    blocks_dev = initial_dictionary_matrix.shape[0] // BS
    width = initial_dictionary_matrix.shape[1]

    def scalar(x):
        return x.reshape(1).astype(i32)

    one_t, two_t = initial_dictionary_matrix.T, decoder_two.T
    sums = squares(one_t, two_t, depth)
    places = (scalar(column), scalar(chip), scalar(core), scalar(1 - core))
    sums, places = tied((sums, places))
    at_column, at_chip, at_core, at_other = places
    sums = lax.all_to_all(sums, AA, 0, 0, tiled=True).sum(axis=0)
    inverse = lax.rsqrt(sums + norm_floor)

    slots = candidate_pair_slots[0].T
    pairs = slots.shape[1]
    first, second = pack(at_column, route_one, route_two, one_t, two_t, inverse, slots)
    first, second = tied((first, second))
    first = lax.all_to_all(first, BA, 0, 0, tiled=True)
    first, second = tied((first, second))
    swap = [(0, 1), (1, 0)]

    def by_chip(a, tiles):
        other = cosines(at_other, slots, a, tiles, first, width)
        other = lax.ppermute(other, "aa_1", swap)
        own = cosines(at_core, slots, a, tiles, first, width)
        return both_cores(at_chip, own, other)

    def to_chips(parts):
        return [parts[0]] + [
            lax.ppermute(parts[d], "aa_0", [(x, (x + d) % 4) for x in range(4)])
            for d in range(1, 4)
        ]

    parts = by_chip(first, (4, 5, 6))
    parts, second = tied((parts, second))
    upper = to_chips(parts)
    second = lax.all_to_all(second, BA, 0, 0, tiled=True)
    parts, second = tied((by_chip(second, (0,)), second))
    lower = to_chips(parts)
    k_upper, t_upper = affinity(upper)
    k_lower, t_lower = affinity(lower)

    def masks():
        every = second[:, width : width + 2, :pairs].astype(i32)
        s_all, r_all = every[:, 0], every[:, 1]

        def block_of(source, route):
            chosen = source[:, :, None] == jnp.arange(owners)[None, None, :]
            return source * blocks_dev + jnp.sum(jnp.where(chosen, route.T[:, None, :], 0), axis=2)

        each = pairs // depth

        def by_device(x):
            x = x.reshape(owners, 2, 4, each)
            return x.transpose(2, 1, 0, 3).reshape(devices, each)

        row_dev, col_dev = by_device(block_of(s_all, route_one)), by_device(block_of(r_all, route_two))
        me = (chip * 2 + core) * owners + column
        pad = jnp.full((4 - each,), -2, i32)
        my_rows = jnp.concatenate([lax.dynamic_index_in_dim(row_dev, me, 0, False), pad])
        my_cols = jnp.concatenate([lax.dynamic_index_in_dim(col_dev, me, 0, False), pad])
        own_blocks = column * blocks_dev + jnp.arange(blocks_dev)
        return [
            hot_rows(my_rows, row_dev),
            hot_rows(my_cols, col_dev),
            hot_rows(own_blocks, row_dev),
            hot_rows(own_blocks, col_dev),
        ]

    hot = masks()

    mats, hot = tied(((k_upper, k_lower, t_upper, t_lower), hot))
    by_row, by_col = mats[2:], mats[:2]
    got = exchanged(step(None, None, by_row, devices))
    for _ in range(SWEEPS - 1):
        got = exchanged(step(got, hot[0], by_col, devices))
        got = exchanged(step(got, hot[1], by_row, devices))
    last = exchanged(step(got, hot[0], by_col, devices))
    got, last = tied((got, last))
    logs = [jax.ShapeDtypeStruct((blocks_dev * TILES, LANES), f32)] * 2
    row_log, col_log = on_chip(log_kernel, logs, 2**20, (got, hot[2], last, hot[3]))
    return row_log.reshape(-1), col_log.reshape(-1)


def solution(mesh):
    torus = Mesh(mesh.devices.reshape(4, 2, 4, 4), ("aa_0", "aa_1", "ba_0", "ba_1"))
    in_specs = (P(BA, AA), P(BA, AA), P(), P(), P(BA, None, None))
    out_specs = (P(BA), P(BA))
    return jax.shard_map(
        per_device, mesh=torus, in_specs=in_specs, out_specs=out_specs, check_vma=False
    )
```

```python
import jax
import jax.numpy as jnp
from jax import lax
from jax.experimental import pallas as pl
from jax.experimental.pallas import tpu as pltpu
from jax.sharding import Mesh
from jax.sharding import PartitionSpec as P

BS = 512
SWEEPS = 4
BA = ("ba_0", "ba_1")
AA = ("aa_0", "aa_1")
ALL = AA + BA
LANES = 128
TILES = BS // LANES
HALF = BS // 2
CHUNKS = (2, 1, 1)
FIXED = 32000.0
IDS = 16


smoothing_regularizer = 0.02
norm_floor = 1e-06

f32, bf16, i16, i32 = jnp.float32, jnp.bfloat16, jnp.int16, jnp.int32


def call(kernel, out_shape, grid_spec, flops, bytes_accessed, args, mebibytes=8):
    return pl.pallas_call(
        kernel,
        out_shape=out_shape,
        grid_spec=grid_spec,
        compiler_params=pltpu.CompilerParams(vmem_limit_bytes=mebibytes * 2**20),
        cost_estimate=pl.CostEstimate(
            flops=flops, bytes_accessed=bytes_accessed, transcendentals=0
        ),
    )(*args)


def squares_kernel(one_ref, two_ref, sums_ref):
    for i, ref in enumerate((one_ref, two_ref)):
        total = jnp.sum(jnp.square(ref[...].astype(f32)), axis=0, keepdims=True)
        sums_ref[:, i : i + 1, :] = jnp.broadcast_to(total[None], (sums_ref.shape[0], 1, BS))


def squares(one, two, depth):
    width, rows = one.shape
    block = pl.BlockSpec((width, BS), lambda k: (0, k))
    spec = pl.GridSpec(
        grid=(rows // BS,),
        in_specs=[block, block],
        out_specs=pl.BlockSpec((depth, 2, BS), lambda k: (0, 0, k)),
    )
    shape = jax.ShapeDtypeStruct((depth, 2, rows), f32)
    return call(squares_kernel, shape, spec, 4 * one.size, 8 * one.size, (one, two), 60)


def pack_kernel(
    me_ref, one_ref, two_ref, a_ref, b_ref, inv_a_ref, inv_b_ref, slots_ref, *out_refs
):
    width, pairs = a_ref.shape[0], slots_ref.shape[1]
    unit_b = (b_ref[...].astype(f32) * inv_b_ref[1:2, :]).astype(bf16)
    unit_a = (a_ref[...].astype(f32) * inv_a_ref[0:1, :]).astype(bf16)
    out_refs[0][0] = unit_b[:, :HALF]
    out_refs[1][0] = unit_b[:, HALF:]
    at = 0
    for ref in out_refs[2:]:
        lanes = ref.shape[2]
        ref[0, :width, :] = unit_a[:, at : at + lanes]
        at += lanes
    last = out_refs[-1]
    last[0, width:, :] = jnp.zeros((IDS, LANES), bf16)
    last[0, width : width + 2, :pairs] = slots_ref[...].astype(f32).astype(bf16)


def pack(me, one, two, a, b, inverse, slots):
    width, owners = a.shape[0], one.shape[0]
    blocks = [(1, width, HALF)] * 2 + [(1, width, n * LANES) for n in CHUNKS]
    blocks[-1] = (1, width + IDS, CHUNKS[-1] * LANES)
    spec = pltpu.PrefetchScalarGridSpec(
        num_scalar_prefetch=3,
        grid=(owners,),
        in_specs=[
            pl.BlockSpec((width, BS), lambda o, me, r1, r2: (0, r1[me[0], o])),
            pl.BlockSpec((width, BS), lambda o, me, r1, r2: (0, r2[me[0], o])),
            pl.BlockSpec((2, BS), lambda o, me, r1, r2: (0, r1[me[0], o])),
            pl.BlockSpec((2, BS), lambda o, me, r1, r2: (0, r2[me[0], o])),
            pl.BlockSpec(slots.shape, lambda o, me, r1, r2: (0, 0)),
        ],
        out_specs=[pl.BlockSpec(x, lambda o, me, r1, r2: (o, 0, 0)) for x in blocks],
    )
    shape = [jax.ShapeDtypeStruct((owners, *x[1:]), bf16) for x in blocks]
    size = owners * width * 2 * BS
    args = (me, one, two, a, b, inverse, inverse, slots)
    return call(pack_kernel, shape, spec, 2 * size, 4 * size, args)


def cosine_kernel(core_ref, slots_ref, a_ref, low_ref, high_ref, out_ref):
    pairs, width = out_ref.shape[0], low_ref.shape[1]

    @pl.loop(0, pairs)
    def _(q):
        at = core_ref[0] * pairs + q
        a = a_ref[slots_ref[0, at], :width, :].T
        for i, ref in enumerate((low_ref, high_ref)):
            partial = jnp.dot(a, ref[slots_ref[1, at]], preferred_element_type=f32)
            fixed = jnp.floor(partial * FIXED + 0.5).astype(i32).astype(i16)
            out_ref[q, :, i * HALF : (i + 1) * HALF] = fixed


def cosines(core, slots, a, low, high):
    pairs, rows = slots.shape[1] // 2, a.shape[2]
    scalars = pl.BlockSpec(memory_space=pltpu.SMEM)
    vectors = pl.BlockSpec(memory_space=pltpu.VMEM)
    flops = 2 * pairs * rows * BS * low.shape[1]
    return pl.pallas_call(
        cosine_kernel,
        out_shape=jax.ShapeDtypeStruct((pairs, rows, BS), i16),
        in_specs=[scalars, scalars, vectors, vectors, vectors],
        out_specs=vectors,
        compiler_params=pltpu.CompilerParams(vmem_limit_bytes=24 * 2**20),
        cost_estimate=pl.CostEstimate(
            flops=flops, bytes_accessed=2 * a.size + 4 * low.size, transcendentals=0
        ),
    )(core, slots, a, low, high)


def both_cores_kernel(x_ref, *refs):
    ins, outs = refs[:8], refs[8:]
    for d in range(4):
        total = ins[d][...].astype(i32) + ins[4 + d][...].astype(i32)
        outs[d][...] = total.astype(i16)


def both_cores(chip, own, other):
    each = own.shape[0] // 4
    block = (1, *own.shape[1:])

    def at(d):
        return pl.BlockSpec(block, lambda k, x: (lax.rem(x[0] + d, 4) * each + k, 0, 0))

    spec = pltpu.PrefetchScalarGridSpec(
        num_scalar_prefetch=1,
        grid=(each,),
        in_specs=[at(d) for d in range(4)] * 2,
        out_specs=[pl.BlockSpec(block, lambda k, x: (k, 0, 0))] * 4,
    )
    shape = [jax.ShapeDtypeStruct((each, *own.shape[1:]), i16)] * 4
    size = own.size
    return call(
        both_cores_kernel, shape, spec, size, 6 * size, (chip, *([own] * 4), *([other] * 4))
    )


def affinity_kernel(a_ref, b_ref, c_ref, d_ref, out_ref, turned_ref):
    total = a_ref[0].astype(i32) + b_ref[0].astype(i32)
    total = total + c_ref[0].astype(i32) + d_ref[0].astype(i32)
    value = jnp.exp(total.astype(f32) * (1.0 / (FIXED * smoothing_regularizer)))
    out_ref[0] = value
    turned_ref[0] = value.T


def affinity(parts):
    each, rows, cols = parts[0].shape
    spec = pl.GridSpec(
        grid=(each,),
        in_specs=[pl.BlockSpec((1, rows, cols), lambda k: (k, 0, 0))] * 4,
        out_specs=[
            pl.BlockSpec((1, rows, cols), lambda k: (k, 0, 0)),
            pl.BlockSpec((1, cols, rows), lambda k: (k, 0, 0)),
        ],
    )
    shape = [
        jax.ShapeDtypeStruct((each, rows, cols), f32),
        jax.ShapeDtypeStruct((each, cols, rows), f32),
    ]
    size = each * rows * cols
    return call(affinity_kernel, shape, spec, 8 * size, 16 * size, tuple(parts))


def emit_rows(rows, out_ref):
    high = [r.astype(bf16).astype(f32) for r in rows]
    low = [r - h for r, h in zip(rows, high)]
    tile = jnp.concatenate(high + low, axis=0).astype(bf16)
    out_ref[...] = jnp.broadcast_to(tile[None], out_ref.shape)


def times_rows(mats, scale):
    turned = None if scale is None else scale.T

    def tile(m, at, k, j):
        part = m[k, at * LANES : (at + 1) * LANES, :]
        if turned is not None:
            part = part * turned[:, TILES * k + j : TILES * k + j + 1]
        return jnp.sum(part, axis=0, keepdims=True)

    rows = []
    for k in range(mats[0].shape[0]):
        if mats[0].shape[1] == BS:
            groups = [[tile(m, j, k, j) for j in range(TILES)] for m in mats]
        else:
            places = [(m, at) for m in mats for at in range(m.shape[1] // LANES)]
            groups = [[tile(m, at, k, j) for j, (m, at) in enumerate(places)]]
        for g in groups:
            total = (g[0] + g[1]) + (g[2] + g[3])
            rows += [total[:, t : t + LANES] for t in range(0, total.shape[1], LANES)]
    return rows


def start_kernel(*refs):
    emit_rows(times_rows(refs[:-1], None), refs[-1])


def totals_of(hot, got_ref):
    got = got_ref[...].reshape(-1, LANES)
    return jnp.dot(hot, got, preferred_element_type=f32)


def step_kernel(got_ref, hot_ref, *refs):
    scale = 1.0 / (1.0 + totals_of(hot_ref[...], got_ref))
    padded = jnp.concatenate([scale, jnp.zeros((LANES - scale.shape[0], LANES), f32)], axis=0)
    emit_rows(times_rows(refs[:-1], padded), refs[-1])


def log_kernel(row_got_ref, row_hot_ref, col_got_ref, col_hot_ref, row_log_ref, col_log_ref):
    row_log_ref[...] = jnp.log(1.0 / (1.0 + totals_of(row_hot_ref[...], row_got_ref)))
    col_log_ref[...] = jnp.log(1.0 / (1.0 + totals_of(col_hot_ref[...], col_got_ref)))


def on_chip(kernel, out_shape, flops, args):
    return pl.pallas_call(
        kernel,
        out_shape=out_shape,
        in_specs=[pl.BlockSpec(memory_space=pltpu.VMEM)] * len(args),
        out_specs=jax.tree.map(lambda _: pl.BlockSpec(memory_space=pltpu.VMEM), out_shape),
        compiler_params=pltpu.CompilerParams(vmem_limit_bytes=8 * 2**20),
        cost_estimate=pl.CostEstimate(flops=flops, bytes_accessed=flops, transcendentals=0),
    )(*args)


def step(got, hot, mats, devices):
    rows = 2 * TILES * mats[0].shape[0]
    out = jax.ShapeDtypeStruct((devices, rows, LANES), bf16)
    flops = 8 * mats[0].size
    if got is None:
        return on_chip(start_kernel, out, flops, tuple(mats))
    return on_chip(step_kernel, out, flops, (got, hot, *mats))


def exchanged(x):
    return lax.all_to_all(x, ALL, 0, 0, tiled=True)


def hot_rows(wanted, present):
    devices, pairs = present.shape
    shape = (devices, 2, pairs, TILES)
    col_id = jnp.broadcast_to(present[:, None, :, None], shape).reshape(1, -1)
    col_tile = lax.broadcasted_iota(i32, shape, 3).reshape(1, -1)
    row_id = jnp.repeat(wanted, TILES)[:, None]
    row_tile = jnp.tile(jnp.arange(TILES), wanted.shape[0])[:, None]
    return ((row_id == col_id) & (row_tile == col_tile)).astype(bf16)


tied = lax.optimization_barrier


def per_device(initial_dictionary_matrix, decoder_two, route_one, route_two, candidate_pair_slots):
    column = lax.axis_index(BA)
    chip = lax.axis_index("aa_0")
    core = lax.axis_index("aa_1")
    owners = lax.axis_size(BA)
    depth = lax.axis_size(AA)
    devices = owners * depth
    blocks_dev = initial_dictionary_matrix.shape[0] // BS
    width = initial_dictionary_matrix.shape[1]

    def scalar(x):
        return x.reshape(1).astype(i32)

    one_t, two_t = initial_dictionary_matrix.T, decoder_two.T
    sums = squares(one_t, two_t, depth)
    places = (scalar(column), scalar(chip), scalar(core), scalar(1 - core))
    sums, places = tied((sums, places))
    at_column, at_chip, at_core, at_other = places
    sums = lax.all_to_all(sums, AA, 0, 0, tiled=True).sum(axis=0)
    inverse = lax.rsqrt(sums + norm_floor)

    slots = candidate_pair_slots[0].T
    pairs = slots.shape[1]
    sent = pack(at_column, route_one, route_two, one_t, two_t, inverse, slots)
    sent = tied(tuple(sent))
    swap = [(0, 1), (1, 0)]
    low, high = None, None

    def gathered(x):
        return lax.all_to_all(x, BA, 0, 0, tiled=True)

    def by_chip(a):
        other = cosines(at_other, slots, a, low, high)
        other = lax.ppermute(other, "aa_1", swap)
        own = cosines(at_core, slots, a, low, high)
        return both_cores(at_chip, own, other)

    def to_chips(parts):
        return [parts[0]] + [
            lax.ppermute(parts[d], "aa_0", [(x, (x + d) % 4) for x in range(4)])
            for d in range(1, 4)
        ]

    low, sent = tied((gathered(sent[0]), sent[1:]))
    high, sent = tied((gathered(sent[0]), sent[1:]))
    spread = []
    for _ in range(len(CHUNKS)):
        a = gathered(sent[0])
        a, sent = tied((a, sent[1:]))
        parts = by_chip(a)
        parts, a, sent = tied((parts, a, sent))
        spread.append(to_chips(parts))
    second = a
    met = [affinity(parts) for parts in spread[:-1]]
    met.append(affinity(spread[-1]))

    def masks():
        every = second[:, width : width + 2, :pairs].astype(i32)
        s_all, r_all = every[:, 0], every[:, 1]

        def block_of(source, route):
            chosen = source[:, :, None] == jnp.arange(owners)[None, None, :]
            return source * blocks_dev + jnp.sum(jnp.where(chosen, route.T[:, None, :], 0), axis=2)

        each = pairs // depth

        def by_device(x):
            x = x.reshape(owners, 2, 4, each)
            return x.transpose(2, 1, 0, 3).reshape(devices, each)

        row_dev, col_dev = by_device(block_of(s_all, route_one)), by_device(block_of(r_all, route_two))
        me = (chip * 2 + core) * owners + column
        pad = jnp.full((4 - each,), -2, i32)
        my_rows = jnp.concatenate([lax.dynamic_index_in_dim(row_dev, me, 0, False), pad])
        my_cols = jnp.concatenate([lax.dynamic_index_in_dim(col_dev, me, 0, False), pad])
        own_blocks = column * blocks_dev + jnp.arange(blocks_dev)
        return [
            hot_rows(my_rows, row_dev),
            hot_rows(my_cols, col_dev),
            hot_rows(own_blocks, row_dev),
            hot_rows(own_blocks, col_dev),
        ]

    hot = masks()

    met, hot = tied((met, hot))
    by_row, by_col = [m[1] for m in met], [m[0] for m in met]
    got = exchanged(step(None, None, by_row, devices))
    for _ in range(SWEEPS - 1):
        got = exchanged(step(got, hot[0], by_col, devices))
        got = exchanged(step(got, hot[1], by_row, devices))
    last = exchanged(step(got, hot[0], by_col, devices))
    got, last = tied((got, last))
    logs = [jax.ShapeDtypeStruct((blocks_dev * TILES, LANES), f32)] * 2
    row_log, col_log = on_chip(log_kernel, logs, 2**20, (got, hot[2], last, hot[3]))
    return row_log.reshape(-1), col_log.reshape(-1)


def solution(mesh):
    torus = Mesh(mesh.devices.reshape(4, 2, 4, 4), ("aa_0", "aa_1", "ba_0", "ba_1"))
    in_specs = (P(BA, AA), P(BA, AA), P(), P(), P(BA, None, None))
    out_specs = (P(BA), P(BA))
    return jax.shard_map(
        per_device, mesh=torus, in_specs=in_specs, out_specs=out_specs, check_vma=False
    )
```

```python
import functools

import jax
import jax.numpy as jnp
from jax import lax
from jax.experimental import pallas as pl
from jax.experimental.pallas import tpu as pltpu
from jax.sharding import Mesh
from jax.sharding import PartitionSpec as P

BS = 512
SWEEPS = 4
BA = ("ba_0", "ba_1")
AA = ("aa_0", "aa_1")
ALL = AA + BA
LANES = 128
TILES = BS // LANES
HALF = BS // 2
CHUNKS = (3, 1)
FIXED = 32000.0
IDS = 16


smoothing_regularizer = 0.02
norm_floor = 1e-06

f32, bf16, i16, i32 = jnp.float32, jnp.bfloat16, jnp.int16, jnp.int32


def call(kernel, out_shape, grid_spec, flops, bytes_accessed, args, mebibytes=8):
    return pl.pallas_call(
        kernel,
        out_shape=out_shape,
        grid_spec=grid_spec,
        compiler_params=pltpu.CompilerParams(vmem_limit_bytes=mebibytes * 2**20),
        cost_estimate=pl.CostEstimate(
            flops=flops, bytes_accessed=bytes_accessed, transcendentals=0
        ),
    )(*args)


def squares_kernel(one_ref, two_ref, sums_ref):
    for i, ref in enumerate((one_ref, two_ref)):
        total = jnp.sum(jnp.square(ref[...].astype(f32)), axis=0, keepdims=True)
        sums_ref[:, i : i + 1, :] = jnp.broadcast_to(total[None], (sums_ref.shape[0], 1, BS))


def squares(one, two, depth):
    width, rows = one.shape
    block = pl.BlockSpec((width, BS), lambda k: (0, k))
    spec = pl.GridSpec(
        grid=(rows // BS,),
        in_specs=[block, block],
        out_specs=pl.BlockSpec((depth, 2, BS), lambda k: (0, 0, k)),
    )
    shape = jax.ShapeDtypeStruct((depth, 2, rows), f32)
    return call(squares_kernel, shape, spec, 4 * one.size, 8 * one.size, (one, two), 60)


def pack_kernel(
    me_ref, one_ref, two_ref, a_ref, b_ref, inv_a_ref, inv_b_ref, slots_ref, *out_refs
):
    width, pairs = a_ref.shape[0], slots_ref.shape[1]
    unit_a = (a_ref[...].astype(f32) * inv_a_ref[0:1, :]).astype(bf16)
    out_refs[0][0, :, :BS] = (b_ref[...].astype(f32) * inv_b_ref[1:2, :]).astype(bf16)
    out_refs[0][0, :, BS:] = unit_a[:, : CHUNKS[0] * LANES]
    out_refs[1][0, :width, :] = unit_a[:, CHUNKS[0] * LANES :]
    last = out_refs[-1]
    last[0, width:, :] = jnp.zeros((IDS, LANES), bf16)
    last[0, width : width + 2, :pairs] = slots_ref[...].astype(f32).astype(bf16)


def pack(me, one, two, a, b, inverse, slots):
    width, owners = a.shape[0], one.shape[0]
    blocks = [
        (1, width, BS + CHUNKS[0] * LANES),
        (1, width + IDS, CHUNKS[1] * LANES),
    ]
    spec = pltpu.PrefetchScalarGridSpec(
        num_scalar_prefetch=3,
        grid=(owners,),
        in_specs=[
            pl.BlockSpec((width, BS), lambda o, me, r1, r2: (0, r1[me[0], o])),
            pl.BlockSpec((width, BS), lambda o, me, r1, r2: (0, r2[me[0], o])),
            pl.BlockSpec((2, BS), lambda o, me, r1, r2: (0, r1[me[0], o])),
            pl.BlockSpec((2, BS), lambda o, me, r1, r2: (0, r2[me[0], o])),
            pl.BlockSpec(slots.shape, lambda o, me, r1, r2: (0, 0)),
        ],
        out_specs=[pl.BlockSpec(x, lambda o, me, r1, r2: (o, 0, 0)) for x in blocks],
    )
    shape = [jax.ShapeDtypeStruct((owners, *x[1:]), bf16) for x in blocks]
    size = owners * width * 2 * BS
    args = (me, one, two, a, b, inverse, inverse, slots)
    return call(pack_kernel, shape, spec, 2 * size, 4 * size, args)


def cosine_kernel(outputs, slots_ref, *refs):
    core_refs, out_refs, refs = refs[:outputs], refs[-outputs:], refs[outputs:-outputs]
    pairs, rows, _ = out_refs[0].shape
    b_ref, a_ref = refs[0], refs[-1]
    start, spare = (BS, 0) if len(refs) == 1 else (0, IDS)
    width = a_ref.shape[1] - spare

    for core_ref, out_ref in zip(core_refs, out_refs):

        @pl.loop(0, pairs)
        def _(q):
            at = core_ref[0] * pairs + q
            a = a_ref[slots_ref[0, at], :width, start : start + rows].T
            for i in range(0, BS, HALF):
                b = b_ref[slots_ref[1, at], :, i : i + HALF]
                partial = jnp.dot(a, b, preferred_element_type=f32)
                fixed = jnp.floor(partial * FIXED + 0.5).astype(i32).astype(i16)
                out_ref[q, :, i : i + HALF] = fixed


def cosines(cores, slots, rows, *arrays):
    pairs, width = slots.shape[1] // 2, arrays[0].shape[1]
    scalars = pl.BlockSpec(memory_space=pltpu.SMEM)
    vectors = pl.BlockSpec(memory_space=pltpu.VMEM)
    flops = 2 * pairs * rows * BS * width * len(cores)
    return pl.pallas_call(
        functools.partial(cosine_kernel, len(cores)),
        out_shape=[jax.ShapeDtypeStruct((pairs, rows, BS), i16)] * len(cores),
        in_specs=[scalars] * (1 + len(cores)) + [vectors] * len(arrays),
        out_specs=[vectors] * len(cores),
        compiler_params=pltpu.CompilerParams(vmem_limit_bytes=8 * 2**20),
        cost_estimate=pl.CostEstimate(flops=flops, bytes_accessed=flops // 256, transcendentals=0),
    )(slots, *cores, *arrays)


def both_cores_kernel(x_ref, *refs):
    ins, outs = refs[:8], refs[8:]
    for d in range(4):
        total = ins[d][...].astype(i32) + ins[4 + d][...].astype(i32)
        outs[d][...] = total.astype(i16)


def both_cores(chip, own, other):
    each = own.shape[0] // 4
    block = (1, *own.shape[1:])

    def at(d):
        return pl.BlockSpec(block, lambda k, x: (lax.rem(x[0] + d, 4) * each + k, 0, 0))

    spec = pltpu.PrefetchScalarGridSpec(
        num_scalar_prefetch=1,
        grid=(each,),
        in_specs=[at(d) for d in range(4)] * 2,
        out_specs=[pl.BlockSpec(block, lambda k, x: (k, 0, 0))] * 4,
    )
    shape = [jax.ShapeDtypeStruct((each, *own.shape[1:]), i16)] * 4
    size = own.size
    return call(
        both_cores_kernel, shape, spec, size, 6 * size, (chip, *([own] * 4), *([other] * 4))
    )


def affinity_kernel(a_ref, b_ref, c_ref, d_ref, out_ref, turned_ref):
    total = a_ref[0].astype(i32) + b_ref[0].astype(i32)
    total = total + c_ref[0].astype(i32) + d_ref[0].astype(i32)
    value = jnp.exp(total.astype(f32) * (1.0 / (FIXED * smoothing_regularizer)))
    out_ref[0] = value
    turned_ref[0] = value.T


def affinity(parts):
    each, rows, cols = parts[0].shape
    spec = pl.GridSpec(
        grid=(each,),
        in_specs=[pl.BlockSpec((1, rows, cols), lambda k: (k, 0, 0))] * 4,
        out_specs=[
            pl.BlockSpec((1, rows, cols), lambda k: (k, 0, 0)),
            pl.BlockSpec((1, cols, rows), lambda k: (k, 0, 0)),
        ],
    )
    shape = [
        jax.ShapeDtypeStruct((each, rows, cols), f32),
        jax.ShapeDtypeStruct((each, cols, rows), f32),
    ]
    size = each * rows * cols
    return call(affinity_kernel, shape, spec, 8 * size, 16 * size, tuple(parts))


def emit_rows(rows, out_ref):
    high = [r.astype(bf16).astype(f32) for r in rows]
    low = [r - h for r, h in zip(rows, high)]
    tile = jnp.concatenate(high + low, axis=0).astype(bf16)
    out_ref[...] = jnp.broadcast_to(tile[None], out_ref.shape)


def times_rows(mats, scale):
    turned = None if scale is None else scale.T

    def tile(m, at, k, j):
        part = m[k, at * LANES : (at + 1) * LANES, :]
        if turned is not None:
            part = part * turned[:, TILES * k + j : TILES * k + j + 1]
        return jnp.sum(part, axis=0, keepdims=True)

    rows = []
    for k in range(mats[0].shape[0]):
        if mats[0].shape[1] == BS:
            groups = [[tile(m, j, k, j) for j in range(TILES)] for m in mats]
        else:
            places = [(m, at) for m in mats for at in range(m.shape[1] // LANES)]
            groups = [[tile(m, at, k, j) for j, (m, at) in enumerate(places)]]
        for g in groups:
            total = (g[0] + g[1]) + (g[2] + g[3])
            rows += [total[:, t : t + LANES] for t in range(0, total.shape[1], LANES)]
    return rows


def start_kernel(*refs):
    emit_rows(times_rows(refs[:-1], None), refs[-1])


def totals_of(hot, got_ref):
    got = got_ref[...].reshape(-1, LANES)
    return jnp.dot(hot, got, preferred_element_type=f32)


def step_kernel(got_ref, hot_ref, *refs):
    scale = 1.0 / (1.0 + totals_of(hot_ref[...], got_ref))
    padded = jnp.concatenate([scale, jnp.zeros((LANES - scale.shape[0], LANES), f32)], axis=0)
    emit_rows(times_rows(refs[:-1], padded), refs[-1])


def log_kernel(row_got_ref, row_hot_ref, col_got_ref, col_hot_ref, row_log_ref, col_log_ref):
    row_log_ref[...] = jnp.log(1.0 / (1.0 + totals_of(row_hot_ref[...], row_got_ref)))
    col_log_ref[...] = jnp.log(1.0 / (1.0 + totals_of(col_hot_ref[...], col_got_ref)))


def on_chip(kernel, out_shape, flops, args):
    return pl.pallas_call(
        kernel,
        out_shape=out_shape,
        in_specs=[pl.BlockSpec(memory_space=pltpu.VMEM)] * len(args),
        out_specs=jax.tree.map(lambda _: pl.BlockSpec(memory_space=pltpu.VMEM), out_shape),
        compiler_params=pltpu.CompilerParams(vmem_limit_bytes=8 * 2**20),
        cost_estimate=pl.CostEstimate(flops=flops, bytes_accessed=flops, transcendentals=0),
    )(*args)


def step(got, hot, mats, devices):
    rows = 2 * TILES * mats[0].shape[0]
    out = jax.ShapeDtypeStruct((devices, rows, LANES), bf16)
    flops = 8 * mats[0].size
    if got is None:
        return on_chip(start_kernel, out, flops, tuple(mats))
    return on_chip(step_kernel, out, flops, (got, hot, *mats))


def exchanged(x):
    return lax.all_to_all(x, ALL, 0, 0, tiled=True)


def hot_rows(wanted, present):
    devices, pairs = present.shape
    shape = (devices, 2, pairs, TILES)
    col_id = jnp.broadcast_to(present[:, None, :, None], shape).reshape(1, -1)
    col_tile = lax.broadcasted_iota(i32, shape, 3).reshape(1, -1)
    row_id = jnp.repeat(wanted, TILES)[:, None]
    row_tile = jnp.tile(jnp.arange(TILES), wanted.shape[0])[:, None]
    return ((row_id == col_id) & (row_tile == col_tile)).astype(bf16)


tied = lax.optimization_barrier


def per_device(initial_dictionary_matrix, decoder_two, route_one, route_two, candidate_pair_slots):
    column = lax.axis_index(BA)
    chip = lax.axis_index("aa_0")
    core = lax.axis_index("aa_1")
    owners = lax.axis_size(BA)
    depth = lax.axis_size(AA)
    devices = owners * depth
    blocks_dev = initial_dictionary_matrix.shape[0] // BS
    width = initial_dictionary_matrix.shape[1]

    def scalar(x):
        return x.reshape(1).astype(i32)

    one_t, two_t = initial_dictionary_matrix.T, decoder_two.T
    sums = squares(one_t, two_t, depth)
    places = (scalar(column), scalar(chip), scalar(core), scalar(1 - core))
    sums, places = tied((sums, places))
    at_column, at_chip, at_core, at_other = places
    sums = lax.all_to_all(sums, AA, 0, 0, tiled=True).sum(axis=0)
    inverse = lax.rsqrt(sums + norm_floor)

    slots = candidate_pair_slots[0].T
    pairs = slots.shape[1]
    sent = pack(at_column, route_one, route_two, one_t, two_t, inverse, slots)
    sent = tied(tuple(sent))
    swap = [(0, 1), (1, 0)]

    def gathered(x):
        return lax.all_to_all(x, BA, 0, 0, tiled=True)

    def by_chip(rows, *arrays):
        if len(arrays) == len(CHUNKS):
            other, own = cosines((at_other, at_core), slots, rows, *arrays)
            other = lax.ppermute(other, "aa_1", swap)
        else:
            (other,) = cosines((at_other,), slots, rows, *arrays)
            other = lax.ppermute(other, "aa_1", swap)
            (own,) = cosines((at_core,), slots, rows, *arrays)
        return both_cores(at_chip, own, other)

    def to_chips(parts):
        return [parts[0]] + [
            lax.ppermute(parts[d], "aa_0", [(x, (x + d) % 4) for x in range(4)])
            for d in range(1, 4)
        ]

    spread, arrived = [], []
    for tiles in CHUNKS:
        a = gathered(sent[0])
        a, sent = tied((a, sent[1:]))
        arrived.append(a)
        parts = by_chip(tiles * LANES, *arrived)
        parts, a, sent = tied((parts, a, sent))
        spread.append(to_chips(parts))
    second = a
    met = [affinity(parts) for parts in spread[:-1]]
    met.append(affinity(spread[-1]))

    def masks():
        every = second[:, width : width + 2, :pairs].astype(i32)
        s_all, r_all = every[:, 0], every[:, 1]

        def block_of(source, route):
            chosen = source[:, :, None] == jnp.arange(owners)[None, None, :]
            return source * blocks_dev + jnp.sum(jnp.where(chosen, route.T[:, None, :], 0), axis=2)

        each = pairs // depth

        def by_device(x):
            x = x.reshape(owners, 2, 4, each)
            return x.transpose(2, 1, 0, 3).reshape(devices, each)

        row_dev, col_dev = by_device(block_of(s_all, route_one)), by_device(block_of(r_all, route_two))
        me = (chip * 2 + core) * owners + column
        pad = jnp.full((4 - each,), -2, i32)
        my_rows = jnp.concatenate([lax.dynamic_index_in_dim(row_dev, me, 0, False), pad])
        my_cols = jnp.concatenate([lax.dynamic_index_in_dim(col_dev, me, 0, False), pad])
        own_blocks = column * blocks_dev + jnp.arange(blocks_dev)
        return [
            hot_rows(my_rows, row_dev),
            hot_rows(my_cols, col_dev),
            hot_rows(own_blocks, row_dev),
            hot_rows(own_blocks, col_dev),
        ]

    hot = masks()

    met, hot = tied((met, hot))
    by_row, by_col = [m[1] for m in met], [m[0] for m in met]
    got = exchanged(step(None, None, by_row, devices))
    for _ in range(SWEEPS - 1):
        got = exchanged(step(got, hot[0], by_col, devices))
        got = exchanged(step(got, hot[1], by_row, devices))
    last = exchanged(step(got, hot[0], by_col, devices))
    got, last = tied((got, last))
    logs = [jax.ShapeDtypeStruct((blocks_dev * TILES, LANES), f32)] * 2
    row_log, col_log = on_chip(log_kernel, logs, 2**20, (got, hot[2], last, hot[3]))
    return row_log.reshape(-1), col_log.reshape(-1)


def solution(mesh):
    torus = Mesh(mesh.devices.reshape(4, 2, 4, 4), ("aa_0", "aa_1", "ba_0", "ba_1"))
    in_specs = (P(BA, AA), P(BA, AA), P(), P(), P(BA, None, None))
    out_specs = (P(BA), P(BA))
    return jax.shard_map(
        per_device, mesh=torus, in_specs=in_specs, out_specs=out_specs, check_vma=False
    )
```

```python
import functools

import jax
import jax.numpy as jnp
from jax import lax
from jax.experimental import pallas as pl
from jax.experimental.pallas import tpu as pltpu
from jax.sharding import Mesh
from jax.sharding import PartitionSpec as P

BS = 512
SWEEPS = 4
BA = ("ba_0", "ba_1")
AA = ("aa_0", "aa_1")
ALL = AA + BA
LANES = 128
TILES = BS // LANES
HALF = BS // 2
CHUNKS = (3, 1)
FIXED = 32000.0
IDS = 16


smoothing_regularizer = 0.02
norm_floor = 1e-06

f32, bf16, i16, i32 = jnp.float32, jnp.bfloat16, jnp.int16, jnp.int32


def call(kernel, out_shape, grid_spec, flops, bytes_accessed, args, mebibytes=8):
    return pl.pallas_call(
        kernel,
        out_shape=out_shape,
        grid_spec=grid_spec,
        compiler_params=pltpu.CompilerParams(vmem_limit_bytes=mebibytes * 2**20),
        cost_estimate=pl.CostEstimate(
            flops=flops, bytes_accessed=bytes_accessed, transcendentals=0
        ),
    )(*args)


def squares_kernel(one_ref, two_ref, sums_ref):
    @pl.when(pl.program_id(0) == 0)
    def _():
        sums_ref[...] = jnp.zeros_like(sums_ref)

    for i, ref in enumerate((one_ref, two_ref)):
        total = jnp.sum(jnp.square(ref[...].astype(f32)), axis=0, keepdims=True)
        sums_ref[:, i : i + 1, :] += jnp.broadcast_to(
            total[None], (sums_ref.shape[0], 1, ref.shape[1])
        )


def squares(one, two, depth):
    width, rows = one.shape
    block = pl.BlockSpec((64, rows), lambda k: (k, 0))
    spec = pl.GridSpec(
        grid=(width // 64,),
        in_specs=[block, block],
        out_specs=pl.BlockSpec((depth, 2, rows), lambda k: (0, 0, 0)),
    )
    shape = jax.ShapeDtypeStruct((depth, 2, rows), f32)
    return call(squares_kernel, shape, spec, 4 * one.size, 8 * one.size, (one, two), 60)


def pack_kernel(
    me_ref, one_ref, two_ref, a_ref, b_ref, inv_a_ref, inv_b_ref, slots_ref, *out_refs
):
    width, pairs = a_ref.shape[0], slots_ref.shape[1]
    unit_a = (a_ref[...].astype(f32) * inv_a_ref[0:1, :]).astype(bf16)
    out_refs[0][0, :, :BS] = (b_ref[...].astype(f32) * inv_b_ref[1:2, :]).astype(bf16)
    out_refs[0][0, :, BS:] = unit_a[:, : CHUNKS[0] * LANES]
    out_refs[1][0, :width, :] = unit_a[:, CHUNKS[0] * LANES :]
    last = out_refs[-1]
    last[0, width:, :] = jnp.zeros((IDS, LANES), bf16)
    last[0, width : width + 2, :pairs] = slots_ref[...].astype(f32).astype(bf16)


def pack(me, one, two, a, b, inverse, slots):
    width, owners = a.shape[0], one.shape[0]
    blocks = [
        (1, width, BS + CHUNKS[0] * LANES),
        (1, width + IDS, CHUNKS[1] * LANES),
    ]
    spec = pltpu.PrefetchScalarGridSpec(
        num_scalar_prefetch=3,
        grid=(owners,),
        in_specs=[
            pl.BlockSpec((width, BS), lambda o, me, r1, r2: (0, r1[me[0], o])),
            pl.BlockSpec((width, BS), lambda o, me, r1, r2: (0, r2[me[0], o])),
            pl.BlockSpec((2, BS), lambda o, me, r1, r2: (0, r1[me[0], o])),
            pl.BlockSpec((2, BS), lambda o, me, r1, r2: (0, r2[me[0], o])),
            pl.BlockSpec(slots.shape, lambda o, me, r1, r2: (0, 0)),
        ],
        out_specs=[pl.BlockSpec(x, lambda o, me, r1, r2: (o, 0, 0)) for x in blocks],
    )
    shape = [jax.ShapeDtypeStruct((owners, *x[1:]), bf16) for x in blocks]
    size = owners * width * 2 * BS
    args = (me, one, two, a, b, inverse, inverse, slots)
    return call(pack_kernel, shape, spec, 2 * size, 4 * size, args)


def cosine_kernel(outputs, slots_ref, *refs):
    core_refs, out_refs, refs = refs[:outputs], refs[-outputs:], refs[outputs:-outputs]
    pairs, rows, _ = out_refs[0].shape
    b_ref, a_ref = refs[0], refs[-1]
    start, spare = (BS, 0) if len(refs) == 1 else (0, IDS)
    width = a_ref.shape[1] - spare

    for core_ref, out_ref in zip(core_refs, out_refs):

        @pl.loop(0, pairs)
        def _(q):
            at = core_ref[0] * pairs + q
            a = a_ref[slots_ref[0, at], :width, start : start + rows].T
            for i in range(0, BS, HALF):
                b = b_ref[slots_ref[1, at], :, i : i + HALF]
                partial = jnp.dot(a, b, preferred_element_type=f32)
                fixed = jnp.floor(partial * FIXED + 0.5).astype(i32).astype(i16)
                out_ref[q, :, i : i + HALF] = fixed


def cosines(cores, slots, rows, *arrays):
    pairs, width = slots.shape[1] // 2, arrays[0].shape[1]
    scalars = pl.BlockSpec(memory_space=pltpu.SMEM)
    vectors = pl.BlockSpec(memory_space=pltpu.VMEM)
    flops = 2 * pairs * rows * BS * width * len(cores)
    return pl.pallas_call(
        functools.partial(cosine_kernel, len(cores)),
        out_shape=[jax.ShapeDtypeStruct((pairs, rows, BS), i16)] * len(cores),
        in_specs=[scalars] * (1 + len(cores)) + [vectors] * len(arrays),
        out_specs=[vectors] * len(cores),
        compiler_params=pltpu.CompilerParams(vmem_limit_bytes=8 * 2**20),
        cost_estimate=pl.CostEstimate(flops=flops, bytes_accessed=flops // 256, transcendentals=0),
    )(slots, *cores, *arrays)


def both_cores_kernel(x_ref, *refs):
    ins, outs = refs[:8], refs[8:]
    for d in range(4):
        total = ins[d][...].astype(i32) + ins[4 + d][...].astype(i32)
        outs[d][...] = total.astype(i16)


def both_cores(chip, own, other):
    each = own.shape[0] // 4
    block = (1, *own.shape[1:])

    def at(d):
        return pl.BlockSpec(block, lambda k, x: (lax.rem(x[0] + d, 4) * each + k, 0, 0))

    spec = pltpu.PrefetchScalarGridSpec(
        num_scalar_prefetch=1,
        grid=(each,),
        in_specs=[at(d) for d in range(4)] * 2,
        out_specs=[pl.BlockSpec(block, lambda k, x: (k, 0, 0))] * 4,
    )
    shape = [jax.ShapeDtypeStruct((each, *own.shape[1:]), i16)] * 4
    size = own.size
    return call(
        both_cores_kernel, shape, spec, size, 6 * size, (chip, *([own] * 4), *([other] * 4))
    )


def affinity_kernel(a_ref, b_ref, c_ref, d_ref, out_ref, turned_ref):
    total = a_ref[0].astype(i32) + b_ref[0].astype(i32)
    total = total + c_ref[0].astype(i32) + d_ref[0].astype(i32)
    value = jnp.exp(total.astype(f32) * (1.0 / (FIXED * smoothing_regularizer)))
    out_ref[0] = value
    turned_ref[0] = value.T


def affinity(parts):
    each, rows, cols = parts[0].shape
    spec = pl.GridSpec(
        grid=(each,),
        in_specs=[pl.BlockSpec((1, rows, cols), lambda k: (k, 0, 0))] * 4,
        out_specs=[
            pl.BlockSpec((1, rows, cols), lambda k: (k, 0, 0)),
            pl.BlockSpec((1, cols, rows), lambda k: (k, 0, 0)),
        ],
    )
    shape = [
        jax.ShapeDtypeStruct((each, rows, cols), f32),
        jax.ShapeDtypeStruct((each, cols, rows), f32),
    ]
    size = each * rows * cols
    return call(affinity_kernel, shape, spec, 8 * size, 16 * size, tuple(parts))


def emit_rows(rows, out_ref):
    high = [r.astype(bf16).astype(f32) for r in rows]
    spare = out_ref.shape[1] - len(rows)
    low = [r - h for r, h in zip(rows, high)]
    if spare < len(rows):
        low = [jnp.zeros((spare, LANES), f32)]
    tile = jnp.concatenate(high + low, axis=0).astype(bf16)
    out_ref[...] = jnp.broadcast_to(tile[None], out_ref.shape)


def times_rows(mats, scale):
    turned = None if scale is None else scale.T

    def tile(m, at, k, j):
        part = m[k, at * LANES : (at + 1) * LANES, :]
        if turned is not None:
            part = part * turned[:, TILES * k + j : TILES * k + j + 1]
        return jnp.sum(part, axis=0, keepdims=True)

    rows = []
    for k in range(mats[0].shape[0]):
        if mats[0].shape[1] == BS:
            groups = [[tile(m, j, k, j) for j in range(TILES)] for m in mats]
        else:
            places = [(m, at) for m in mats for at in range(m.shape[1] // LANES)]
            groups = [[tile(m, at, k, j) for j, (m, at) in enumerate(places)]]
        for g in groups:
            total = (g[0] + g[1]) + (g[2] + g[3])
            rows += [total[:, t : t + LANES] for t in range(0, total.shape[1], LANES)]
    return rows


def start_kernel(*refs):
    emit_rows(times_rows(refs[:-1], None), refs[-1])


def totals_of(hot, got_ref):
    got = got_ref[...].reshape(-1, LANES)
    return jnp.dot(hot, got, preferred_element_type=f32)


def step_kernel(got_ref, hot_ref, *refs):
    scale = 1.0 / (1.0 + totals_of(hot_ref[...], got_ref))
    padded = jnp.concatenate([scale, jnp.zeros((LANES - scale.shape[0], LANES), f32)], axis=0)
    emit_rows(times_rows(refs[:-1], padded), refs[-1])


def log_kernel(row_got_ref, row_hot_ref, col_got_ref, col_hot_ref, row_log_ref, col_log_ref):
    row_log_ref[...] = jnp.log(1.0 / (1.0 + totals_of(row_hot_ref[...], row_got_ref)))
    col_log_ref[...] = jnp.log(1.0 / (1.0 + totals_of(col_hot_ref[...], col_got_ref)))


def on_chip(kernel, out_shape, flops, args):
    return pl.pallas_call(
        kernel,
        out_shape=out_shape,
        in_specs=[pl.BlockSpec(memory_space=pltpu.VMEM)] * len(args),
        out_specs=jax.tree.map(lambda _: pl.BlockSpec(memory_space=pltpu.VMEM), out_shape),
        compiler_params=pltpu.CompilerParams(vmem_limit_bytes=8 * 2**20),
        cost_estimate=pl.CostEstimate(flops=flops, bytes_accessed=flops, transcendentals=0),
    )(*args)


def step(got, hot, mats, devices, fine=True):
    pairs = mats[0].shape[0]
    rows = TILES * (2 * pairs if fine else pairs + 1)
    out = jax.ShapeDtypeStruct((devices, rows, LANES), bf16)
    flops = 8 * mats[0].size
    if got is None:
        return on_chip(start_kernel, out, flops, tuple(mats))
    return on_chip(step_kernel, out, flops, (got, hot, *mats))


def exchanged(x):
    return lax.all_to_all(x, ALL, 0, 0, tiled=True)


def hot_rows(wanted, present, fine=True):
    devices, pairs = present.shape
    if not fine:
        present = jnp.concatenate([present, jnp.full((devices, 1), -1, i32)], axis=1)
    shape = (devices, 2, pairs, TILES) if fine else (devices, 1, pairs + 1, TILES)
    col_id = jnp.broadcast_to(present[:, None, :, None], shape).reshape(1, -1)
    col_tile = lax.broadcasted_iota(i32, shape, 3).reshape(1, -1)
    row_id = jnp.repeat(wanted, TILES)[:, None]
    row_tile = jnp.tile(jnp.arange(TILES), wanted.shape[0])[:, None]
    return ((row_id == col_id) & (row_tile == col_tile)).astype(bf16)


tied = lax.optimization_barrier


def per_device(initial_dictionary_matrix, decoder_two, route_one, route_two, candidate_pair_slots):
    column = lax.axis_index(BA)
    chip = lax.axis_index("aa_0")
    core = lax.axis_index("aa_1")
    owners = lax.axis_size(BA)
    depth = lax.axis_size(AA)
    devices = owners * depth
    blocks_dev = initial_dictionary_matrix.shape[0] // BS
    width = initial_dictionary_matrix.shape[1]

    def scalar(x):
        return x.reshape(1).astype(i32)

    one_t, two_t = initial_dictionary_matrix.T, decoder_two.T
    sums = squares(one_t, two_t, depth)
    places = (scalar(column), scalar(chip), scalar(core), scalar(1 - core))
    sums, places = tied((sums, places))
    at_column, at_chip, at_core, at_other = places
    sums = lax.all_to_all(sums, AA, 0, 0, tiled=True).sum(axis=0)
    inverse = lax.rsqrt(sums + norm_floor)

    slots = candidate_pair_slots[0].T
    pairs = slots.shape[1]
    sent = pack(at_column, route_one, route_two, one_t, two_t, inverse, slots)
    sent = tied(tuple(sent))
    swap = [(0, 1), (1, 0)]

    def gathered(x):
        return lax.all_to_all(x, BA, 0, 0, tiled=True)

    def by_chip(rows, *arrays):
        if len(arrays) == len(CHUNKS):
            other, own = cosines((at_other, at_core), slots, rows, *arrays)
            other = lax.ppermute(other, "aa_1", swap)
        else:
            (other,) = cosines((at_other,), slots, rows, *arrays)
            other = lax.ppermute(other, "aa_1", swap)
            (own,) = cosines((at_core,), slots, rows, *arrays)
        return both_cores(at_chip, own, other)

    def to_chips(parts):
        return [parts[0]] + [
            lax.ppermute(parts[d], "aa_0", [(x, (x + d) % 4) for x in range(4)])
            for d in range(1, 4)
        ]

    spread, arrived = [], []
    for tiles in CHUNKS:
        a = gathered(sent[0])
        a, sent = tied((a, sent[1:]))
        arrived.append(a)
        parts = by_chip(tiles * LANES, *arrived)
        parts, a, sent = tied((parts, a, sent))
        spread.append(to_chips(parts))
    second = a
    met = [affinity(parts) for parts in spread[:-1]]
    met.append(affinity(spread[-1]))

    def masks():
        every = second[:, width : width + 2, :pairs].astype(i32)
        s_all, r_all = every[:, 0], every[:, 1]

        def block_of(source, route):
            chosen = source[:, :, None] == jnp.arange(owners)[None, None, :]
            return source * blocks_dev + jnp.sum(jnp.where(chosen, route.T[:, None, :], 0), axis=2)

        each = pairs // depth

        def by_device(x):
            x = x.reshape(owners, 2, 4, each)
            return x.transpose(2, 1, 0, 3).reshape(devices, each)

        row_dev, col_dev = by_device(block_of(s_all, route_one)), by_device(block_of(r_all, route_two))
        me = (chip * 2 + core) * owners + column
        pad = jnp.full((4 - each,), -2, i32)
        my_rows = jnp.concatenate([lax.dynamic_index_in_dim(row_dev, me, 0, False), pad])
        my_cols = jnp.concatenate([lax.dynamic_index_in_dim(col_dev, me, 0, False), pad])
        own_blocks = column * blocks_dev + jnp.arange(blocks_dev)
        return [
            hot_rows(my_rows, row_dev),
            hot_rows(my_cols, col_dev),
            hot_rows(own_blocks, row_dev),
            hot_rows(own_blocks, col_dev),
            hot_rows(my_rows, row_dev, False),
            hot_rows(my_cols, col_dev, False),
        ]

    hot = masks()

    met, hot = tied((met, hot))
    by_row, by_col = [m[1] for m in met], [m[0] for m in met]
    got = exchanged(step(None, None, by_row, devices, False))
    got = exchanged(step(got, hot[4], by_col, devices, False))
    got = exchanged(step(got, hot[5], by_row, devices))
    for _ in range(SWEEPS - 2):
        got = exchanged(step(got, hot[0], by_col, devices))
        got = exchanged(step(got, hot[1], by_row, devices))
    last = exchanged(step(got, hot[0], by_col, devices))
    got, last = tied((got, last))
    logs = [jax.ShapeDtypeStruct((blocks_dev * TILES, LANES), f32)] * 2
    row_log, col_log = on_chip(log_kernel, logs, 2**20, (got, hot[2], last, hot[3]))
    return row_log.reshape(-1), col_log.reshape(-1)


def solution(mesh):
    torus = Mesh(mesh.devices.reshape(4, 2, 4, 4), ("aa_0", "aa_1", "ba_0", "ba_1"))
    in_specs = (P(BA, AA), P(BA, AA), P(), P(), P(BA, None, None))
    out_specs = (P(BA), P(BA))
    return jax.shard_map(
        per_device, mesh=torus, in_specs=in_specs, out_specs=out_specs, check_vma=False
    )
```

```python
import functools

import jax
import jax.numpy as jnp
from jax import lax
from jax.experimental import pallas as pl
from jax.experimental.pallas import tpu as pltpu
from jax.sharding import Mesh
from jax.sharding import PartitionSpec as P

BS = 512
SWEEPS = 4
BA = ("ba_0", "ba_1")
AA = ("aa_0", "aa_1")
CROSSED = ("ba_1", "ba_0")
ALL = ("ba_0", "ba_1", "aa_1", "aa_0")
LANES = 128
TILES = BS // LANES
HALF = BS // 2
CHUNKS = (3, 1)
FIXED = 32000.0
IDS = 16


smoothing_regularizer = 0.02
norm_floor = 1e-06

f32, bf16, i16, i32 = jnp.float32, jnp.bfloat16, jnp.int16, jnp.int32


def crossed(owner):
    return lax.rem(owner, 4) * 4 + lax.div(owner, 4)


def call(kernel, out_shape, grid_spec, flops, bytes_accessed, args, mebibytes=8):
    return pl.pallas_call(
        kernel,
        out_shape=out_shape,
        grid_spec=grid_spec,
        compiler_params=pltpu.CompilerParams(vmem_limit_bytes=mebibytes * 2**20),
        cost_estimate=pl.CostEstimate(
            flops=flops, bytes_accessed=bytes_accessed, transcendentals=0
        ),
    )(*args)


def squares_kernel(one_ref, two_ref, sums_ref):
    @pl.when(pl.program_id(0) == 0)
    def _():
        sums_ref[...] = jnp.zeros_like(sums_ref)

    for i, ref in enumerate((one_ref, two_ref)):
        total = jnp.sum(jnp.square(ref[...].astype(f32)), axis=0, keepdims=True)
        sums_ref[:, i : i + 1, :] += jnp.broadcast_to(
            total[None], (sums_ref.shape[0], 1, ref.shape[1])
        )


def squares(one, two, depth):
    width, rows = one.shape
    block = pl.BlockSpec((64, rows), lambda k: (k, 0))
    spec = pl.GridSpec(
        grid=(width // 64,),
        in_specs=[block, block],
        out_specs=pl.BlockSpec((depth, 2, rows), lambda k: (0, 0, 0)),
    )
    shape = jax.ShapeDtypeStruct((depth, 2, rows), f32)
    return call(squares_kernel, shape, spec, 4 * one.size, 8 * one.size, (one, two), 52)


def pack_kernel(
    me_ref, one_ref, two_ref, a_ref, b_ref, inv_a_ref, inv_b_ref, slots_ref, *out_refs
):
    width, pairs = a_ref.shape[0], slots_ref.shape[1]
    unit_a = (a_ref[...].astype(f32) * inv_a_ref[0:1, :]).astype(bf16)
    out_refs[0][0, :, :BS] = (b_ref[...].astype(f32) * inv_b_ref[1:2, :]).astype(bf16)
    out_refs[0][0, :, BS:] = unit_a[:, : CHUNKS[0] * LANES]
    out_refs[1][0, :width, :] = unit_a[:, CHUNKS[0] * LANES :]
    last = out_refs[-1]
    last[0, width:, :] = jnp.zeros((IDS, LANES), bf16)
    last[0, width : width + 2, :pairs] = slots_ref[...].astype(f32).astype(bf16)


def pack(me, one, two, a, b, inverse, slots):
    width, owners = a.shape[0], one.shape[0]
    blocks = [
        (1, width, BS + CHUNKS[0] * LANES),
        (1, width + IDS, CHUNKS[1] * LANES),
    ]
    spec = pltpu.PrefetchScalarGridSpec(
        num_scalar_prefetch=3,
        grid=(owners,),
        in_specs=[
            pl.BlockSpec((width, BS), lambda o, me, r1, r2: (0, r1[me[0], crossed(o)])),
            pl.BlockSpec((width, BS), lambda o, me, r1, r2: (0, r2[me[0], crossed(o)])),
            pl.BlockSpec((2, BS), lambda o, me, r1, r2: (0, r1[me[0], crossed(o)])),
            pl.BlockSpec((2, BS), lambda o, me, r1, r2: (0, r2[me[0], crossed(o)])),
            pl.BlockSpec(slots.shape, lambda o, me, r1, r2: (0, 0)),
        ],
        out_specs=[pl.BlockSpec(x, lambda o, me, r1, r2: (o, 0, 0)) for x in blocks],
    )
    shape = [jax.ShapeDtypeStruct((owners, *x[1:]), bf16) for x in blocks]
    size = owners * width * 2 * BS
    args = (me, one, two, a, b, inverse, inverse, slots)
    return call(pack_kernel, shape, spec, 2 * size, 4 * size, args)


def cosine_kernel(outputs, slots_ref, *refs):
    core_refs, out_refs, refs = refs[:outputs], refs[-outputs:], refs[outputs:-outputs]
    pairs, rows, _ = out_refs[0].shape
    b_ref, a_ref = refs[0], refs[-1]
    start, spare = (BS, 0) if len(refs) == 1 else (0, IDS)
    width = a_ref.shape[1] - spare

    for core_ref, out_ref in zip(core_refs, out_refs):

        @pl.loop(0, pairs)
        def _(q):
            at = core_ref[0] * pairs + q
            a = a_ref[crossed(slots_ref[0, at]), :width, start : start + rows].T
            for i in range(0, BS, HALF):
                b = b_ref[crossed(slots_ref[1, at]), :, i : i + HALF]
                partial = jnp.dot(a, b, preferred_element_type=f32)
                fixed = jnp.floor(partial * FIXED + 0.5).astype(i32).astype(i16)
                out_ref[q, :, i : i + HALF] = fixed


def cosines(cores, slots, rows, *arrays):
    pairs, width = slots.shape[1] // 2, arrays[0].shape[1]
    scalars = pl.BlockSpec(memory_space=pltpu.SMEM)
    vectors = pl.BlockSpec(memory_space=pltpu.VMEM)
    flops = 2 * pairs * rows * BS * width * len(cores)
    return pl.pallas_call(
        functools.partial(cosine_kernel, len(cores)),
        out_shape=[jax.ShapeDtypeStruct((pairs, rows, BS), i16)] * len(cores),
        in_specs=[scalars] * (1 + len(cores)) + [vectors] * len(arrays),
        out_specs=[vectors] * len(cores),
        compiler_params=pltpu.CompilerParams(vmem_limit_bytes=8 * 2**20),
        cost_estimate=pl.CostEstimate(flops=flops, bytes_accessed=flops // 256, transcendentals=0),
    )(slots, *cores, *arrays)


def both_cores_kernel(x_ref, *refs):
    ins, outs = refs[:8], refs[8:]
    for d in range(4):
        total = ins[d][...].astype(i32) + ins[4 + d][...].astype(i32)
        outs[d][...] = total.astype(i16)


def both_cores(chip, own, other):
    each = own.shape[0] // 4
    block = (1, *own.shape[1:])

    def at(d):
        return pl.BlockSpec(block, lambda k, x: (lax.rem(x[0] + d, 4) * each + k, 0, 0))

    spec = pltpu.PrefetchScalarGridSpec(
        num_scalar_prefetch=1,
        grid=(each,),
        in_specs=[at(d) for d in range(4)] * 2,
        out_specs=[pl.BlockSpec(block, lambda k, x: (k, 0, 0))] * 4,
    )
    shape = [jax.ShapeDtypeStruct((each, *own.shape[1:]), i16)] * 4
    size = own.size
    return call(
        both_cores_kernel, shape, spec, size, 6 * size, (chip, *([own] * 4), *([other] * 4))
    )


def affinity_kernel(a_ref, b_ref, c_ref, d_ref, out_ref, turned_ref):
    total = a_ref[0].astype(i32) + b_ref[0].astype(i32)
    total = total + c_ref[0].astype(i32) + d_ref[0].astype(i32)
    value = jnp.exp(total.astype(f32) * (1.0 / (FIXED * smoothing_regularizer)))
    out_ref[0] = value
    turned_ref[0] = value.T


def affinity(parts):
    each, rows, cols = parts[0].shape
    spec = pl.GridSpec(
        grid=(each,),
        in_specs=[pl.BlockSpec((1, rows, cols), lambda k: (k, 0, 0))] * 4,
        out_specs=[
            pl.BlockSpec((1, rows, cols), lambda k: (k, 0, 0)),
            pl.BlockSpec((1, cols, rows), lambda k: (k, 0, 0)),
        ],
    )
    shape = [
        jax.ShapeDtypeStruct((each, rows, cols), f32),
        jax.ShapeDtypeStruct((each, cols, rows), f32),
    ]
    size = each * rows * cols
    return call(affinity_kernel, shape, spec, 8 * size, 16 * size, tuple(parts))


def emit_rows(rows, out_ref):
    high = [r.astype(bf16).astype(f32) for r in rows]
    spare = out_ref.shape[1] - len(rows)
    low = [r - h for r, h in zip(rows, high)]
    if spare < len(rows):
        low = [jnp.zeros((spare, LANES), f32)]
    tile = jnp.concatenate(high + low, axis=0).astype(bf16)
    out_ref[...] = jnp.broadcast_to(tile[None], out_ref.shape)


def times_rows(mats, scale):
    turned = None if scale is None else scale.T

    def tile(m, at, k, j):
        part = m[k, at * LANES : (at + 1) * LANES, :]
        if turned is not None:
            part = part * turned[:, TILES * k + j : TILES * k + j + 1]
        return jnp.sum(part, axis=0, keepdims=True)

    rows = []
    for k in range(mats[0].shape[0]):
        if mats[0].shape[1] == BS:
            groups = [[tile(m, j, k, j) for j in range(TILES)] for m in mats]
        else:
            places = [(m, at) for m in mats for at in range(m.shape[1] // LANES)]
            groups = [[tile(m, at, k, j) for j, (m, at) in enumerate(places)]]
        for g in groups:
            total = (g[0] + g[1]) + (g[2] + g[3])
            rows += [total[:, t : t + LANES] for t in range(0, total.shape[1], LANES)]
    return rows


def start_kernel(*refs):
    emit_rows(times_rows(refs[:-1], None), refs[-1])


def totals_of(hot, got_ref):
    got = got_ref[...].reshape(-1, LANES)
    return jnp.dot(hot, got, preferred_element_type=f32)


def step_kernel(got_ref, hot_ref, *refs):
    scale = 1.0 / (1.0 + totals_of(hot_ref[...], got_ref))
    padded = jnp.concatenate([scale, jnp.zeros((LANES - scale.shape[0], LANES), f32)], axis=0)
    emit_rows(times_rows(refs[:-1], padded), refs[-1])


def log_kernel(row_got_ref, row_hot_ref, col_got_ref, col_hot_ref, row_log_ref, col_log_ref):
    row_log_ref[...] = jnp.log(1.0 / (1.0 + totals_of(row_hot_ref[...], row_got_ref)))
    col_log_ref[...] = jnp.log(1.0 / (1.0 + totals_of(col_hot_ref[...], col_got_ref)))


def on_chip(kernel, out_shape, flops, args):
    return pl.pallas_call(
        kernel,
        out_shape=out_shape,
        in_specs=[pl.BlockSpec(memory_space=pltpu.VMEM)] * len(args),
        out_specs=jax.tree.map(lambda _: pl.BlockSpec(memory_space=pltpu.VMEM), out_shape),
        compiler_params=pltpu.CompilerParams(vmem_limit_bytes=8 * 2**20),
        cost_estimate=pl.CostEstimate(flops=flops, bytes_accessed=flops, transcendentals=0),
    )(*args)


def step(got, hot, mats, devices, fine=True):
    pairs = mats[0].shape[0]
    rows = TILES * (2 * pairs if fine else pairs + 1)
    out = jax.ShapeDtypeStruct((devices, rows, LANES), bf16)
    flops = 8 * mats[0].size
    if got is None:
        return on_chip(start_kernel, out, flops, tuple(mats))
    return on_chip(step_kernel, out, flops, (got, hot, *mats))


def exchanged(x):
    return lax.all_to_all(x, ALL, 0, 0, tiled=True)


def hot_rows(wanted, present, fine=True):
    devices, pairs = present.shape
    if not fine:
        present = jnp.concatenate([present, jnp.full((devices, 1), -1, i32)], axis=1)
    shape = (devices, 2, pairs, TILES) if fine else (devices, 1, pairs + 1, TILES)
    col_id = jnp.broadcast_to(present[:, None, :, None], shape).reshape(1, -1)
    col_tile = lax.broadcasted_iota(i32, shape, 3).reshape(1, -1)
    row_id = jnp.repeat(wanted, TILES)[:, None]
    row_tile = jnp.tile(jnp.arange(TILES), wanted.shape[0])[:, None]
    return ((row_id == col_id) & (row_tile == col_tile)).astype(bf16)


tied = lax.optimization_barrier


def per_device(initial_dictionary_matrix, decoder_two, route_one, route_two, candidate_pair_slots):
    column = lax.axis_index(BA)
    chip = lax.axis_index("aa_0")
    core = lax.axis_index("aa_1")
    owners = lax.axis_size(BA)
    depth = lax.axis_size(AA)
    devices = owners * depth
    blocks_dev = initial_dictionary_matrix.shape[0] // BS
    width = initial_dictionary_matrix.shape[1]

    def scalar(x):
        return x.reshape(1).astype(i32)

    one_t, two_t = initial_dictionary_matrix.T, decoder_two.T
    sums = squares(one_t, two_t, depth)
    places = (scalar(column), scalar(chip), scalar(core), scalar(1 - core))
    sums, places = tied((sums, places))
    at_column, at_chip, at_core, at_other = places
    sums = lax.all_to_all(sums, AA, 0, 0, tiled=True).sum(axis=0)
    inverse = lax.rsqrt(sums + norm_floor)

    slots = candidate_pair_slots[0].T
    pairs = slots.shape[1]
    sent = pack(at_column, route_one, route_two, one_t, two_t, inverse, slots)
    sent = tied(tuple(sent))
    swap = [(0, 1), (1, 0)]

    def gathered(x):
        return lax.all_to_all(x, CROSSED, 0, 0, tiled=True)

    def by_chip(rows, *arrays):
        if len(arrays) == len(CHUNKS):
            other, own = cosines((at_other, at_core), slots, rows, *arrays)
            other = lax.ppermute(other, "aa_1", swap)
        else:
            (other,) = cosines((at_other,), slots, rows, *arrays)
            other = lax.ppermute(other, "aa_1", swap)
            (own,) = cosines((at_core,), slots, rows, *arrays)
        return both_cores(at_chip, own, other)

    def to_chips(parts):
        return [parts[0]] + [
            lax.ppermute(parts[d], "aa_0", [(x, (x + d) % 4) for x in range(4)])
            for d in range(1, 4)
        ]

    spread, arrived = [], []
    for tiles in CHUNKS:
        a = gathered(sent[0])
        a, sent = tied((a, sent[1:]))
        arrived.append(a)
        parts = by_chip(tiles * LANES, *arrived)
        parts, a, sent = tied((parts, a, sent))
        spread.append(to_chips(parts))
    second = a
    met = [affinity(parts) for parts in spread[:-1]]
    met.append(affinity(spread[-1]))

    def masks():
        every = second[:, width : width + 2, :pairs].astype(i32)
        every = every.reshape(4, 4, 2, pairs).swapaxes(0, 1).reshape(owners, 2, pairs)
        s_all, r_all = every[:, 0], every[:, 1]

        def block_of(source, route):
            chosen = source[:, :, None] == jnp.arange(owners)[None, None, :]
            return source * blocks_dev + jnp.sum(jnp.where(chosen, route.T[:, None, :], 0), axis=2)

        each = pairs // depth

        def by_device(x):
            return x.reshape(devices, each)

        row_dev, col_dev = by_device(block_of(s_all, route_one)), by_device(block_of(r_all, route_two))
        me = (column * 2 + core) * 4 + chip
        pad = jnp.full((4 - each,), -2, i32)
        my_rows = jnp.concatenate([lax.dynamic_index_in_dim(row_dev, me, 0, False), pad])
        my_cols = jnp.concatenate([lax.dynamic_index_in_dim(col_dev, me, 0, False), pad])
        own_blocks = column * blocks_dev + jnp.arange(blocks_dev)
        return [
            hot_rows(my_rows, row_dev),
            hot_rows(my_cols, col_dev),
            hot_rows(own_blocks, row_dev),
            hot_rows(own_blocks, col_dev),
            hot_rows(my_rows, row_dev, False),
            hot_rows(my_cols, col_dev, False),
        ]

    hot = masks()

    met, hot = tied((met, hot))
    by_row, by_col = [m[1] for m in met], [m[0] for m in met]
    got = exchanged(step(None, None, by_row, devices, False))
    got = exchanged(step(got, hot[4], by_col, devices, False))
    got = exchanged(step(got, hot[5], by_row, devices))
    for _ in range(SWEEPS - 2):
        got = exchanged(step(got, hot[0], by_col, devices))
        got = exchanged(step(got, hot[1], by_row, devices))
    last = exchanged(step(got, hot[0], by_col, devices))
    got, last = tied((got, last))
    logs = [jax.ShapeDtypeStruct((blocks_dev * TILES, LANES), f32)] * 2
    row_log, col_log = on_chip(log_kernel, logs, 2**20, (got, hot[2], last, hot[3]))
    return row_log.reshape(-1), col_log.reshape(-1)


def solution(mesh):
    torus = Mesh(mesh.devices.reshape(4, 2, 4, 4), ("aa_0", "aa_1", "ba_0", "ba_1"))
    in_specs = (P(BA, AA), P(BA, AA), P(), P(), P(BA, None, None))
    out_specs = (P(BA), P(BA))
    return jax.shard_map(
        per_device, mesh=torus, in_specs=in_specs, out_specs=out_specs, check_vma=False
    )
```

```python
import functools

import jax
import jax.numpy as jnp
from jax import lax
from jax.experimental import pallas as pl
from jax.experimental.pallas import tpu as pltpu
from jax.sharding import Mesh
from jax.sharding import PartitionSpec as P

BS = 512
SWEEPS = 4
BA = ("ba_0", "ba_1")
AA = ("aa_0", "aa_1")
CROSSED = ("ba_1", "ba_0")
ALL = ("ba_0", "ba_1", "aa_1", "aa_0")
LANES = 128
TILES = BS // LANES
HALF = BS // 2
CHUNKS = (3, 1)
FIXED = 32000.0
IDS = 16


smoothing_regularizer = 0.02
norm_floor = 1e-06

f32, bf16, i16, i32 = jnp.float32, jnp.bfloat16, jnp.int16, jnp.int32


def crossed(owner):
    return lax.rem(owner, 4) * 4 + lax.div(owner, 4)


def call(kernel, out_shape, grid_spec, flops, bytes_accessed, args, mebibytes=8):
    return pl.pallas_call(
        kernel,
        out_shape=out_shape,
        grid_spec=grid_spec,
        compiler_params=pltpu.CompilerParams(vmem_limit_bytes=mebibytes * 2**20),
        cost_estimate=pl.CostEstimate(
            flops=flops, bytes_accessed=bytes_accessed, transcendentals=0
        ),
    )(*args)


def squares_kernel(one_ref, two_ref, sums_ref):
    @pl.when(pl.program_id(0) == 0)
    def _():
        sums_ref[...] = jnp.zeros_like(sums_ref)

    for i, ref in enumerate((one_ref, two_ref)):
        total = jnp.sum(jnp.square(ref[...].astype(f32)), axis=0, keepdims=True)
        sums_ref[:, i : i + 1, :] += jnp.broadcast_to(
            total[None], (sums_ref.shape[0], 1, ref.shape[1])
        )


def squares(one, two, depth):
    width, rows = one.shape
    block = pl.BlockSpec((64, rows), lambda k: (k, 0))
    spec = pl.GridSpec(
        grid=(width // 64,),
        in_specs=[block, block],
        out_specs=pl.BlockSpec((depth, 2, rows), lambda k: (0, 0, 0)),
    )
    shape = jax.ShapeDtypeStruct((depth, 2, rows), f32)
    return call(squares_kernel, shape, spec, 4 * one.size, 8 * one.size, (one, two), 52)


def pack_kernel(
    me_ref, one_ref, two_ref, a_ref, b_ref, inv_a_ref, inv_b_ref, slots_ref, *out_refs
):
    width, pairs = a_ref.shape[0], slots_ref.shape[1]
    unit_a = (a_ref[...].astype(f32) * inv_a_ref[0:1, :]).astype(bf16)
    out_refs[0][0, :, :BS] = (b_ref[...].astype(f32) * inv_b_ref[1:2, :]).astype(bf16)
    out_refs[0][0, :, BS:] = unit_a[:, : CHUNKS[0] * LANES]
    out_refs[1][0, :width, :] = unit_a[:, CHUNKS[0] * LANES :]
    last = out_refs[-1]
    last[0, width:, :] = jnp.zeros((IDS, LANES), bf16)
    last[0, width : width + 2, :pairs] = slots_ref[...].astype(f32).astype(bf16)


def pack(me, one, two, a, b, inverse, slots):
    width, owners = a.shape[0], one.shape[0]
    blocks = [
        (1, width, BS + CHUNKS[0] * LANES),
        (1, width + IDS, CHUNKS[1] * LANES),
    ]
    spec = pltpu.PrefetchScalarGridSpec(
        num_scalar_prefetch=3,
        grid=(owners,),
        in_specs=[
            pl.BlockSpec((width, BS), lambda o, me, r1, r2: (0, r1[me[0], crossed(o)])),
            pl.BlockSpec((width, BS), lambda o, me, r1, r2: (0, r2[me[0], crossed(o)])),
            pl.BlockSpec((2, BS), lambda o, me, r1, r2: (0, r1[me[0], crossed(o)])),
            pl.BlockSpec((2, BS), lambda o, me, r1, r2: (0, r2[me[0], crossed(o)])),
            pl.BlockSpec(slots.shape, lambda o, me, r1, r2: (0, 0)),
        ],
        out_specs=[pl.BlockSpec(x, lambda o, me, r1, r2: (o, 0, 0)) for x in blocks],
    )
    shape = [jax.ShapeDtypeStruct((owners, *x[1:]), bf16) for x in blocks]
    size = owners * width * 2 * BS
    args = (me, one, two, a, b, inverse, inverse, slots)
    return call(pack_kernel, shape, spec, 2 * size, 4 * size, args)


def cosine_kernel(outputs, slots_ref, *refs):
    core_refs, out_refs, refs = refs[:outputs], refs[-outputs:], refs[outputs:-outputs]
    pairs, rows, _ = out_refs[0].shape
    b_ref, a_ref = refs[0], refs[-1]
    start, spare = (BS, 0) if len(refs) == 1 else (0, IDS)
    width = a_ref.shape[1] - spare

    for core_ref, out_ref in zip(core_refs, out_refs):

        @pl.loop(0, pairs)
        def _(q):
            at = core_ref[0] * pairs + q
            a = a_ref[crossed(slots_ref[0, at]), :width, start : start + rows].T
            for i in range(0, BS, HALF):
                b = b_ref[crossed(slots_ref[1, at]), :, i : i + HALF]
                partial = jnp.dot(a, b, preferred_element_type=f32)
                fixed = jnp.floor(partial * FIXED + 0.5).astype(i32).astype(i16)
                out_ref[q, :, i : i + HALF] = fixed


def cosines(cores, slots, rows, *arrays):
    pairs, width = slots.shape[1] // 2, arrays[0].shape[1]
    scalars = pl.BlockSpec(memory_space=pltpu.SMEM)
    vectors = pl.BlockSpec(memory_space=pltpu.VMEM)
    flops = 2 * pairs * rows * BS * width * len(cores)
    return pl.pallas_call(
        functools.partial(cosine_kernel, len(cores)),
        out_shape=[jax.ShapeDtypeStruct((pairs, rows, BS), i16)] * len(cores),
        in_specs=[scalars] * (1 + len(cores)) + [vectors] * len(arrays),
        out_specs=[vectors] * len(cores),
        compiler_params=pltpu.CompilerParams(vmem_limit_bytes=8 * 2**20),
        cost_estimate=pl.CostEstimate(flops=flops, bytes_accessed=flops // 256, transcendentals=0),
    )(slots, *cores, *arrays)


def both_cores_kernel(x_ref, *refs):
    ins, outs = refs[:8], refs[8:]
    for d in range(4):
        total = ins[d][...].astype(i32) + ins[4 + d][...].astype(i32)
        outs[d][...] = total.astype(i16)


def both_cores(chip, own, other):
    each = own.shape[0] // 4
    block = (1, *own.shape[1:])

    def at(d):
        return pl.BlockSpec(block, lambda k, x: (lax.rem(x[0] + d, 4) * each + k, 0, 0))

    spec = pltpu.PrefetchScalarGridSpec(
        num_scalar_prefetch=1,
        grid=(each,),
        in_specs=[at(d) for d in range(4)] * 2,
        out_specs=[pl.BlockSpec(block, lambda k, x: (k, 0, 0))] * 4,
    )
    shape = [jax.ShapeDtypeStruct((each, *own.shape[1:]), i16)] * 4
    size = own.size
    return call(
        both_cores_kernel, shape, spec, size, 6 * size, (chip, *([own] * 4), *([other] * 4))
    )


def affinity_kernel(a_ref, b_ref, c_ref, d_ref, out_ref, turned_ref):
    total = a_ref[0].astype(i32) + b_ref[0].astype(i32)
    total = total + c_ref[0].astype(i32) + d_ref[0].astype(i32)
    value = jnp.exp(total.astype(f32) * (1.0 / (FIXED * smoothing_regularizer)))
    out_ref[0] = value
    turned_ref[0] = value.T


def affinity(parts):
    each, rows, cols = parts[0].shape
    spec = pl.GridSpec(
        grid=(each,),
        in_specs=[pl.BlockSpec((1, rows, cols), lambda k: (k, 0, 0))] * 4,
        out_specs=[
            pl.BlockSpec((1, rows, cols), lambda k: (k, 0, 0)),
            pl.BlockSpec((1, cols, rows), lambda k: (k, 0, 0)),
        ],
    )
    shape = [
        jax.ShapeDtypeStruct((each, rows, cols), f32),
        jax.ShapeDtypeStruct((each, cols, rows), f32),
    ]
    size = each * rows * cols
    return call(affinity_kernel, shape, spec, 8 * size, 16 * size, tuple(parts))


def emit_rows(rows, out_ref):
    high = [r.astype(bf16).astype(f32) for r in rows]
    spare = out_ref.shape[1] - len(rows)
    low = [r - h for r, h in zip(rows, high)]
    if spare < len(rows):
        low = [jnp.zeros((spare, LANES), f32)]
    tile = jnp.concatenate(high + low, axis=0).astype(bf16)
    out_ref[...] = jnp.broadcast_to(tile[None], out_ref.shape)


def times_rows(mats, scale):
    turned = None if scale is None else scale.T

    def tile(m, at, k, j):
        part = m[k, at * LANES : (at + 1) * LANES, :]
        if turned is not None:
            part = part * turned[:, TILES * k + j : TILES * k + j + 1]
        return jnp.sum(part, axis=0, keepdims=True)

    rows = []
    for k in range(mats[0].shape[0]):
        if mats[0].shape[1] == BS:
            groups = [[tile(m, j, k, j) for j in range(TILES)] for m in mats]
        else:
            places = [(m, at) for m in mats for at in range(m.shape[1] // LANES)]
            groups = [[tile(m, at, k, j) for j, (m, at) in enumerate(places)]]
        for g in groups:
            total = (g[0] + g[1]) + (g[2] + g[3])
            rows += [total[:, t : t + LANES] for t in range(0, total.shape[1], LANES)]
    return rows


def start_kernel(*refs):
    emit_rows(times_rows(refs[:-1], None), refs[-1])


def totals_of(hot, got_ref):
    got = got_ref[...].reshape(-1, LANES)
    return jnp.dot(hot, got, preferred_element_type=f32)


def step_kernel(got_ref, hot_ref, *refs):
    scale = 1.0 / (1.0 + totals_of(hot_ref[...], got_ref))
    padded = jnp.concatenate([scale, jnp.zeros((LANES - scale.shape[0], LANES), f32)], axis=0)
    emit_rows(times_rows(refs[:-1], padded), refs[-1])


def last_kernel(core_ref, chip_ref, slots_ref, got_ref, hot_ref, *refs):
    mats, out_ref = refs[:-1], refs[-1]
    scale = 1.0 / (1.0 + totals_of(hot_ref[...], got_ref))
    padded = jnp.concatenate([scale, jnp.zeros((LANES - scale.shape[0], LANES), f32)], axis=0)
    rows = times_rows(mats, padded)
    each = mats[0].shape[0]
    totals = [jnp.concatenate(rows[TILES * k : TILES * (k + 1)], axis=0) for k in range(each)]
    first = core_ref[0] * (slots_ref.shape[1] // 2) + chip_ref[0] * each
    depth = 2 * 4
    for source in range(out_ref.shape[0] // depth):
        total = jnp.zeros_like(totals[0])
        for k in range(each):
            total = total + jnp.where(slots_ref[1, first + k] == source, totals[k], 0.0)
        high = total.astype(bf16).astype(f32)
        tile = jnp.concatenate([high, total - high], axis=0).astype(bf16)
        out_ref[source * depth : (source + 1) * depth] = jnp.broadcast_to(
            tile[None], (depth, *tile.shape)
        )


def last_step(core, chip, slots, got, hot, mats, devices):
    out = jax.ShapeDtypeStruct((devices, 2 * TILES, LANES), bf16)
    scalars = pl.BlockSpec(memory_space=pltpu.SMEM)
    vectors = pl.BlockSpec(memory_space=pltpu.VMEM)
    return pl.pallas_call(
        last_kernel,
        out_shape=out,
        in_specs=[scalars] * 3 + [vectors] * (2 + len(mats)),
        out_specs=vectors,
        compiler_params=pltpu.CompilerParams(vmem_limit_bytes=8 * 2**20),
    )(core, chip, slots, got, hot, *mats)


def log_kernel(row_got_ref, row_hot_ref, col_got_ref, col_hot_ref, row_log_ref, col_log_ref):
    row_log_ref[...] = jnp.log(1.0 / (1.0 + totals_of(row_hot_ref[...], row_got_ref)))
    col_log_ref[...] = jnp.log(1.0 / (1.0 + totals_of(col_hot_ref[...], col_got_ref)))


def on_chip(kernel, out_shape, flops, args):
    return pl.pallas_call(
        kernel,
        out_shape=out_shape,
        in_specs=[pl.BlockSpec(memory_space=pltpu.VMEM)] * len(args),
        out_specs=jax.tree.map(lambda _: pl.BlockSpec(memory_space=pltpu.VMEM), out_shape),
        compiler_params=pltpu.CompilerParams(vmem_limit_bytes=8 * 2**20),
        cost_estimate=pl.CostEstimate(flops=flops, bytes_accessed=flops, transcendentals=0),
    )(*args)


def step(got, hot, mats, devices, fine=True):
    pairs = mats[0].shape[0]
    rows = TILES * (2 * pairs if fine else pairs + 1)
    out = jax.ShapeDtypeStruct((devices, rows, LANES), bf16)
    flops = 8 * mats[0].size
    if got is None:
        return on_chip(start_kernel, out, flops, tuple(mats))
    return on_chip(step_kernel, out, flops, (got, hot, *mats))


def exchanged(x):
    return lax.all_to_all(x, ALL, 0, 0, tiled=True)


def hot_rows(wanted, present, fine=True):
    devices, pairs = present.shape
    if not fine:
        present = jnp.concatenate([present, jnp.full((devices, 1), -1, i32)], axis=1)
    shape = (devices, 2, pairs, TILES) if fine else (devices, 1, pairs + 1, TILES)
    col_id = jnp.broadcast_to(present[:, None, :, None], shape).reshape(1, -1)
    col_tile = lax.broadcasted_iota(i32, shape, 3).reshape(1, -1)
    row_id = jnp.repeat(wanted, TILES)[:, None]
    row_tile = jnp.tile(jnp.arange(TILES), wanted.shape[0])[:, None]
    return ((row_id == col_id) & (row_tile == col_tile)).astype(bf16)


tied = lax.optimization_barrier


def per_device(initial_dictionary_matrix, decoder_two, route_one, route_two, candidate_pair_slots):
    column = lax.axis_index(BA)
    chip = lax.axis_index("aa_0")
    core = lax.axis_index("aa_1")
    owners = lax.axis_size(BA)
    depth = lax.axis_size(AA)
    devices = owners * depth
    blocks_dev = initial_dictionary_matrix.shape[0] // BS
    width = initial_dictionary_matrix.shape[1]

    def scalar(x):
        return x.reshape(1).astype(i32)

    one_t, two_t = initial_dictionary_matrix.T, decoder_two.T
    sums = squares(one_t, two_t, depth)
    places = (scalar(column), scalar(chip), scalar(core), scalar(1 - core))
    sums, places = tied((sums, places))
    at_column, at_chip, at_core, at_other = places
    sums = lax.all_to_all(sums, AA, 0, 0, tiled=True).sum(axis=0)
    inverse = lax.rsqrt(sums + norm_floor)

    slots = candidate_pair_slots[0].T
    pairs = slots.shape[1]
    sent = pack(at_column, route_one, route_two, one_t, two_t, inverse, slots)
    sent = tied(tuple(sent))
    swap = [(0, 1), (1, 0)]

    def gathered(x):
        return lax.all_to_all(x, CROSSED, 0, 0, tiled=True)

    def by_chip(rows, *arrays):
        if len(arrays) == len(CHUNKS):
            other, own = cosines((at_other, at_core), slots, rows, *arrays)
            other = lax.ppermute(other, "aa_1", swap)
        else:
            (other,) = cosines((at_other,), slots, rows, *arrays)
            other = lax.ppermute(other, "aa_1", swap)
            (own,) = cosines((at_core,), slots, rows, *arrays)
        return both_cores(at_chip, own, other)

    def to_chips(parts):
        return [parts[0]] + [
            lax.ppermute(parts[d], "aa_0", [(x, (x + d) % 4) for x in range(4)])
            for d in range(1, 4)
        ]

    spread, arrived = [], []
    for tiles in CHUNKS:
        a = gathered(sent[0])
        a, sent = tied((a, sent[1:]))
        arrived.append(a)
        parts = by_chip(tiles * LANES, *arrived)
        parts, a, sent = tied((parts, a, sent))
        spread.append(to_chips(parts))
    second = a
    met = [affinity(parts) for parts in spread[:-1]]
    met.append(affinity(spread[-1]))

    def masks():
        every = second[:, width : width + 2, :pairs].astype(i32)
        every = every.reshape(4, 4, 2, pairs).swapaxes(0, 1).reshape(owners, 2, pairs)
        s_all, r_all = every[:, 0], every[:, 1]

        def block_of(source, route):
            chosen = source[:, :, None] == jnp.arange(owners)[None, None, :]
            return source * blocks_dev + jnp.sum(jnp.where(chosen, route.T[:, None, :], 0), axis=2)

        each = pairs // depth

        def by_device(x):
            return x.reshape(devices, each)

        row_dev, col_dev = by_device(block_of(s_all, route_one)), by_device(block_of(r_all, route_two))
        me = (column * 2 + core) * 4 + chip
        pad = jnp.full((4 - each,), -2, i32)
        my_rows = jnp.concatenate([lax.dynamic_index_in_dim(row_dev, me, 0, False), pad])
        my_cols = jnp.concatenate([lax.dynamic_index_in_dim(col_dev, me, 0, False), pad])
        own_blocks = column * blocks_dev + jnp.arange(blocks_dev)
        own_route = lax.dynamic_index_in_dim(route_two, column, 0, False)
        return [
            hot_rows(my_rows, row_dev),
            hot_rows(my_cols, col_dev),
            hot_rows(own_blocks, row_dev),
            hot_rows(jnp.arange(blocks_dev), jnp.repeat(own_route, depth)[:, None]),
            hot_rows(my_rows, row_dev, False),
            hot_rows(my_cols, col_dev, False),
        ]

    hot = masks()

    met, hot = tied((met, hot))
    by_row, by_col = [m[1] for m in met], [m[0] for m in met]
    got = exchanged(step(None, None, by_row, devices, False))
    got = exchanged(step(got, hot[4], by_col, devices, False))
    got = exchanged(step(got, hot[5], by_row, devices))
    for _ in range(SWEEPS - 2):
        got = exchanged(step(got, hot[0], by_col, devices))
        got = exchanged(step(got, hot[1], by_row, devices))
    last = exchanged(last_step(at_core, at_chip, slots, got, hot[0], by_col, devices))
    got, last = tied((got, last))
    logs = [jax.ShapeDtypeStruct((blocks_dev * TILES, LANES), f32)] * 2
    row_log, col_log = on_chip(log_kernel, logs, 2**20, (got, hot[2], last, hot[3]))
    return row_log.reshape(-1), col_log.reshape(-1)


def solution(mesh):
    torus = Mesh(mesh.devices.reshape(4, 2, 4, 4), ("aa_0", "aa_1", "ba_0", "ba_1"))
    in_specs = (P(BA, AA), P(BA, AA), P(), P(), P(BA, None, None))
    out_specs = (P(BA), P(BA))
    return jax.shard_map(
        per_device, mesh=torus, in_specs=in_specs, out_specs=out_specs, check_vma=False
    )
```

```python
import functools

import jax
import jax.numpy as jnp
from jax import lax
from jax.experimental import pallas as pl
from jax.experimental.pallas import tpu as pltpu
from jax.sharding import Mesh
from jax.sharding import PartitionSpec as P

BS = 512
SWEEPS = 4
BA = ("ba_0", "ba_1")
AA = ("aa_0", "aa_1")
CROSSED = ("ba_1", "ba_0")
ALL = ("ba_0", "ba_1", "aa_1", "aa_0")
LANES = 128
TILES = BS // LANES
HALF = BS // 2
CHUNKS = (3, 1)
FIXED = 32000.0
IDS = 16


smoothing_regularizer = 0.02
norm_floor = 1e-06

f32, bf16, i16, i32 = jnp.float32, jnp.bfloat16, jnp.int16, jnp.int32


def crossed(owner):
    return lax.rem(owner, 4) * 4 + lax.div(owner, 4)


def call(kernel, out_shape, grid_spec, flops, bytes_accessed, args, mebibytes=8):
    return pl.pallas_call(
        kernel,
        out_shape=out_shape,
        grid_spec=grid_spec,
        compiler_params=pltpu.CompilerParams(vmem_limit_bytes=mebibytes * 2**20),
        cost_estimate=pl.CostEstimate(
            flops=flops, bytes_accessed=bytes_accessed, transcendentals=0
        ),
    )(*args)


def squares_kernel(one_ref, two_ref, sums_ref):
    @pl.when(pl.program_id(0) == 0)
    def _():
        sums_ref[...] = jnp.zeros_like(sums_ref)

    for i, ref in enumerate((one_ref, two_ref)):
        total = jnp.sum(jnp.square(ref[...].astype(f32)), axis=0, keepdims=True)
        sums_ref[:, i : i + 1, :] += jnp.broadcast_to(
            total[None], (sums_ref.shape[0], 1, ref.shape[1])
        )


def squares(one, two, depth):
    width, rows = one.shape
    block = pl.BlockSpec((32, rows), lambda k: (k, 0))
    spec = pl.GridSpec(
        grid=(width // 32,),
        in_specs=[block, block],
        out_specs=pl.BlockSpec((depth, 2, rows), lambda k: (0, 0, 0)),
    )
    shape = jax.ShapeDtypeStruct((depth, 2, rows), f32)
    return call(squares_kernel, shape, spec, 4 * one.size, 8 * one.size, (one, two), 52)


def pack_kernel(
    me_ref, one_ref, two_ref, a_ref, b_ref, inv_a_ref, inv_b_ref, slots_ref, *out_refs
):
    width, pairs = a_ref.shape[0], slots_ref.shape[1]
    unit_a = (a_ref[...].astype(f32) * inv_a_ref[0:1, :]).astype(bf16)
    out_refs[0][0, :, :BS] = (b_ref[...].astype(f32) * inv_b_ref[1:2, :]).astype(bf16)
    out_refs[0][0, :, BS:] = unit_a[:, : CHUNKS[0] * LANES]
    out_refs[1][0, :width, :] = unit_a[:, CHUNKS[0] * LANES :]
    last = out_refs[-1]
    last[0, width:, :] = jnp.zeros((IDS, LANES), bf16)
    last[0, width : width + 2, :pairs] = slots_ref[...].astype(f32).astype(bf16)


def pack(me, one, two, a, b, inverse, slots):
    width, owners = a.shape[0], one.shape[0]
    blocks = [
        (1, width, BS + CHUNKS[0] * LANES),
        (1, width + IDS, CHUNKS[1] * LANES),
    ]
    spec = pltpu.PrefetchScalarGridSpec(
        num_scalar_prefetch=3,
        grid=(owners,),
        in_specs=[
            pl.BlockSpec((width, BS), lambda o, me, r1, r2: (0, r1[me[0], crossed(o)])),
            pl.BlockSpec((width, BS), lambda o, me, r1, r2: (0, r2[me[0], crossed(o)])),
            pl.BlockSpec((2, BS), lambda o, me, r1, r2: (0, r1[me[0], crossed(o)])),
            pl.BlockSpec((2, BS), lambda o, me, r1, r2: (0, r2[me[0], crossed(o)])),
            pl.BlockSpec(slots.shape, lambda o, me, r1, r2: (0, 0)),
        ],
        out_specs=[pl.BlockSpec(x, lambda o, me, r1, r2: (o, 0, 0)) for x in blocks],
    )
    shape = [jax.ShapeDtypeStruct((owners, *x[1:]), bf16) for x in blocks]
    size = owners * width * 2 * BS
    args = (me, one, two, a, b, inverse, inverse, slots)
    return call(pack_kernel, shape, spec, 2 * size, 4 * size, args)


def cosine_kernel(outputs, slots_ref, *refs):
    core_refs, out_refs, refs = refs[:outputs], refs[-outputs:], refs[outputs:-outputs]
    pairs, rows, _ = out_refs[0].shape
    b_ref, a_ref = refs[0], refs[-1]
    start, spare = (BS, 0) if len(refs) == 1 else (0, IDS)
    width = a_ref.shape[1] - spare

    for core_ref, out_ref in zip(core_refs, out_refs):

        @pl.loop(0, pairs)
        def _(q):
            at = core_ref[0] * pairs + q
            a = a_ref[crossed(slots_ref[0, at]), :width, start : start + rows].T
            for i in range(0, BS, HALF):
                b = b_ref[crossed(slots_ref[1, at]), :, i : i + HALF]
                partial = jnp.dot(a, b, preferred_element_type=f32)
                fixed = jnp.floor(partial * FIXED + 0.5).astype(i32).astype(i16)
                out_ref[q, :, i : i + HALF] = fixed


def cosines(cores, slots, rows, *arrays):
    pairs, width = slots.shape[1] // 2, arrays[0].shape[1]
    scalars = pl.BlockSpec(memory_space=pltpu.SMEM)
    vectors = pl.BlockSpec(memory_space=pltpu.VMEM)
    flops = 2 * pairs * rows * BS * width * len(cores)
    return pl.pallas_call(
        functools.partial(cosine_kernel, len(cores)),
        out_shape=[jax.ShapeDtypeStruct((pairs, rows, BS), i16)] * len(cores),
        in_specs=[scalars] * (1 + len(cores)) + [vectors] * len(arrays),
        out_specs=[vectors] * len(cores),
        compiler_params=pltpu.CompilerParams(vmem_limit_bytes=8 * 2**20),
        cost_estimate=pl.CostEstimate(flops=flops, bytes_accessed=flops // 256, transcendentals=0),
    )(slots, *cores, *arrays)


def both_cores_kernel(x_ref, *refs):
    ins, outs = refs[:8], refs[8:]
    for d in range(4):
        total = ins[d][...].astype(i32) + ins[4 + d][...].astype(i32)
        outs[d][...] = total.astype(i16)


def both_cores(chip, own, other):
    each = own.shape[0] // 4
    block = (1, *own.shape[1:])

    def at(d):
        return pl.BlockSpec(block, lambda k, x: (lax.rem(x[0] + d, 4) * each + k, 0, 0))

    spec = pltpu.PrefetchScalarGridSpec(
        num_scalar_prefetch=1,
        grid=(each,),
        in_specs=[at(d) for d in range(4)] * 2,
        out_specs=[pl.BlockSpec(block, lambda k, x: (k, 0, 0))] * 4,
    )
    shape = [jax.ShapeDtypeStruct((each, *own.shape[1:]), i16)] * 4
    size = own.size
    return call(
        both_cores_kernel, shape, spec, size, 6 * size, (chip, *([own] * 4), *([other] * 4))
    )


def affinity_kernel(a_ref, b_ref, c_ref, d_ref, out_ref, turned_ref):
    total = a_ref[0].astype(i32) + b_ref[0].astype(i32)
    total = total + c_ref[0].astype(i32) + d_ref[0].astype(i32)
    value = jnp.exp(total.astype(f32) * (1.0 / (FIXED * smoothing_regularizer)))
    out_ref[0] = value
    turned_ref[0] = value.T


def affinity(parts):
    each, rows, cols = parts[0].shape
    spec = pl.GridSpec(
        grid=(each,),
        in_specs=[pl.BlockSpec((1, rows, cols), lambda k: (k, 0, 0))] * 4,
        out_specs=[
            pl.BlockSpec((1, rows, cols), lambda k: (k, 0, 0)),
            pl.BlockSpec((1, cols, rows), lambda k: (k, 0, 0)),
        ],
    )
    shape = [
        jax.ShapeDtypeStruct((each, rows, cols), f32),
        jax.ShapeDtypeStruct((each, cols, rows), f32),
    ]
    size = each * rows * cols
    return call(affinity_kernel, shape, spec, 8 * size, 16 * size, tuple(parts))


def emit_rows(rows, out_ref):
    high = [r.astype(bf16).astype(f32) for r in rows]
    spare = out_ref.shape[1] - len(rows)
    low = [r - h for r, h in zip(rows, high)]
    if spare < len(rows):
        low = [jnp.zeros((spare, LANES), f32)]
    tile = jnp.concatenate(high + low, axis=0).astype(bf16)
    out_ref[...] = jnp.broadcast_to(tile[None], out_ref.shape)


def times_rows(mats, scale):
    turned = None if scale is None else scale.T

    def tile(m, at, k, j):
        part = m[k, at * LANES : (at + 1) * LANES, :]
        if turned is not None:
            part = part * turned[:, TILES * k + j : TILES * k + j + 1]
        return jnp.sum(part, axis=0, keepdims=True)

    rows = []
    for k in range(mats[0].shape[0]):
        if mats[0].shape[1] == BS:
            groups = [[tile(m, j, k, j) for j in range(TILES)] for m in mats]
        else:
            places = [(m, at) for m in mats for at in range(m.shape[1] // LANES)]
            groups = [[tile(m, at, k, j) for j, (m, at) in enumerate(places)]]
        for g in groups:
            total = (g[0] + g[1]) + (g[2] + g[3])
            rows += [total[:, t : t + LANES] for t in range(0, total.shape[1], LANES)]
    return rows


def start_kernel(*refs):
    emit_rows(times_rows(refs[:-1], None), refs[-1])


def totals_of(hot, got_ref):
    got = got_ref[...].reshape(-1, LANES)
    return jnp.dot(hot, got, preferred_element_type=f32)


def step_kernel(got_ref, hot_ref, *refs):
    scale = 1.0 / (1.0 + totals_of(hot_ref[...], got_ref))
    padded = jnp.concatenate([scale, jnp.zeros((LANES - scale.shape[0], LANES), f32)], axis=0)
    emit_rows(times_rows(refs[:-1], padded), refs[-1])


def last_kernel(core_ref, chip_ref, slots_ref, got_ref, hot_ref, *refs):
    mats, out_ref = refs[:-1], refs[-1]
    scale = 1.0 / (1.0 + totals_of(hot_ref[...], got_ref))
    padded = jnp.concatenate([scale, jnp.zeros((LANES - scale.shape[0], LANES), f32)], axis=0)
    rows = times_rows(mats, padded)
    each = mats[0].shape[0]
    totals = [jnp.concatenate(rows[TILES * k : TILES * (k + 1)], axis=0) for k in range(each)]
    first = core_ref[0] * (slots_ref.shape[1] // 2) + chip_ref[0] * each
    depth = 2 * 4
    for source in range(out_ref.shape[0] // depth):
        total = jnp.zeros_like(totals[0])
        for k in range(each):
            total = total + jnp.where(slots_ref[1, first + k] == source, totals[k], 0.0)
        high = total.astype(bf16).astype(f32)
        tile = jnp.concatenate([high, total - high], axis=0).astype(bf16)
        out_ref[source * depth : (source + 1) * depth] = jnp.broadcast_to(
            tile[None], (depth, *tile.shape)
        )


def last_step(core, chip, slots, got, hot, mats, devices):
    out = jax.ShapeDtypeStruct((devices, 2 * TILES, LANES), bf16)
    scalars = pl.BlockSpec(memory_space=pltpu.SMEM)
    vectors = pl.BlockSpec(memory_space=pltpu.VMEM)
    return pl.pallas_call(
        last_kernel,
        out_shape=out,
        in_specs=[scalars] * 3 + [vectors] * (2 + len(mats)),
        out_specs=vectors,
        compiler_params=pltpu.CompilerParams(vmem_limit_bytes=8 * 2**20),
    )(core, chip, slots, got, hot, *mats)


def log_kernel(row_got_ref, row_hot_ref, col_got_ref, col_hot_ref, row_log_ref, col_log_ref):
    row_log_ref[...] = jnp.log(1.0 / (1.0 + totals_of(row_hot_ref[...], row_got_ref)))
    col_log_ref[...] = jnp.log(1.0 / (1.0 + totals_of(col_hot_ref[...], col_got_ref)))


def on_chip(kernel, out_shape, flops, args):
    return pl.pallas_call(
        kernel,
        out_shape=out_shape,
        in_specs=[pl.BlockSpec(memory_space=pltpu.VMEM)] * len(args),
        out_specs=jax.tree.map(lambda _: pl.BlockSpec(memory_space=pltpu.VMEM), out_shape),
        compiler_params=pltpu.CompilerParams(vmem_limit_bytes=8 * 2**20),
        cost_estimate=pl.CostEstimate(flops=flops, bytes_accessed=flops, transcendentals=0),
    )(*args)


def step(got, hot, mats, devices, fine=True):
    pairs = mats[0].shape[0]
    rows = TILES * (2 * pairs if fine else pairs + 1)
    out = jax.ShapeDtypeStruct((devices, rows, LANES), bf16)
    flops = 8 * mats[0].size
    if got is None:
        return on_chip(start_kernel, out, flops, tuple(mats))
    return on_chip(step_kernel, out, flops, (got, hot, *mats))


def exchanged(x):
    return lax.all_to_all(x, ALL, 0, 0, tiled=True)


def hot_rows(wanted, present, fine=True):
    devices, pairs = present.shape
    if not fine:
        present = jnp.concatenate([present, jnp.full((devices, 1), -1, i32)], axis=1)
    shape = (devices, 2, pairs, TILES) if fine else (devices, 1, pairs + 1, TILES)
    col_id = jnp.broadcast_to(present[:, None, :, None], shape).reshape(1, -1)
    col_tile = lax.broadcasted_iota(i32, shape, 3).reshape(1, -1)
    row_id = jnp.repeat(wanted, TILES)[:, None]
    row_tile = jnp.tile(jnp.arange(TILES), wanted.shape[0])[:, None]
    return ((row_id == col_id) & (row_tile == col_tile)).astype(bf16)


tied = lax.optimization_barrier


def per_device(initial_dictionary_matrix, decoder_two, route_one, route_two, candidate_pair_slots):
    column = lax.axis_index(BA)
    chip = lax.axis_index("aa_0")
    core = lax.axis_index("aa_1")
    owners = lax.axis_size(BA)
    depth = lax.axis_size(AA)
    devices = owners * depth
    blocks_dev = initial_dictionary_matrix.shape[0] // BS
    width = initial_dictionary_matrix.shape[1]

    def scalar(x):
        return x.reshape(1).astype(i32)

    one_t, two_t = initial_dictionary_matrix.T, decoder_two.T
    sums = squares(one_t, two_t, depth)
    places = (scalar(column), scalar(chip), scalar(core), scalar(1 - core))
    sums, places = tied((sums, places))
    at_column, at_chip, at_core, at_other = places
    sums = lax.all_to_all(sums, AA, 0, 0, tiled=True).sum(axis=0)
    inverse = lax.rsqrt(sums + norm_floor)

    slots = candidate_pair_slots[0].T
    pairs = slots.shape[1]
    sent = pack(at_column, route_one, route_two, one_t, two_t, inverse, slots)
    sent = tied(tuple(sent))
    swap = [(0, 1), (1, 0)]

    def gathered(x):
        return lax.all_to_all(x, CROSSED, 0, 0, tiled=True)

    def by_chip(rows, *arrays):
        if len(arrays) == len(CHUNKS):
            other, own = cosines((at_other, at_core), slots, rows, *arrays)
            other = lax.ppermute(other, "aa_1", swap)
        else:
            (other,) = cosines((at_other,), slots, rows, *arrays)
            other = lax.ppermute(other, "aa_1", swap)
            (own,) = cosines((at_core,), slots, rows, *arrays)
        return both_cores(at_chip, own, other)

    def to_chips(parts):
        return [parts[0]] + [
            lax.ppermute(parts[d], "aa_0", [(x, (x + d) % 4) for x in range(4)])
            for d in (2, 1, 3)
        ]

    spread, arrived = [], []
    for tiles in CHUNKS:
        a = gathered(sent[0])
        a, sent = tied((a, sent[1:]))
        arrived.append(a)
        parts = by_chip(tiles * LANES, *arrived)
        parts, a, sent = tied((parts, a, sent))
        spread.append(to_chips(parts))
    second = a
    met = [affinity(parts) for parts in spread[:-1]]
    met.append(affinity(spread[-1]))

    def masks():
        every = second[:, width : width + 2, :pairs].astype(i32)
        every = every.reshape(4, 4, 2, pairs).swapaxes(0, 1).reshape(owners, 2, pairs)
        s_all, r_all = every[:, 0], every[:, 1]

        def block_of(source, route):
            chosen = source[:, :, None] == jnp.arange(owners)[None, None, :]
            return source * blocks_dev + jnp.sum(jnp.where(chosen, route.T[:, None, :], 0), axis=2)

        each = pairs // depth

        def by_device(x):
            return x.reshape(devices, each)

        row_dev, col_dev = by_device(block_of(s_all, route_one)), by_device(block_of(r_all, route_two))
        me = (column * 2 + core) * 4 + chip
        pad = jnp.full((4 - each,), -2, i32)
        my_rows = jnp.concatenate([lax.dynamic_index_in_dim(row_dev, me, 0, False), pad])
        my_cols = jnp.concatenate([lax.dynamic_index_in_dim(col_dev, me, 0, False), pad])
        own_blocks = column * blocks_dev + jnp.arange(blocks_dev)
        own_route = lax.dynamic_index_in_dim(route_two, column, 0, False)
        return [
            hot_rows(my_rows, row_dev),
            hot_rows(my_cols, col_dev),
            hot_rows(own_blocks, row_dev),
            hot_rows(jnp.arange(blocks_dev), jnp.repeat(own_route, depth)[:, None]),
            hot_rows(my_rows, row_dev, False),
            hot_rows(my_cols, col_dev, False),
        ]

    hot = masks()

    met, hot = tied((met, hot))
    by_row, by_col = [m[1] for m in met], [m[0] for m in met]
    got = exchanged(step(None, None, by_row, devices, False))
    got = exchanged(step(got, hot[4], by_col, devices, False))
    got = exchanged(step(got, hot[5], by_row, devices))
    for _ in range(SWEEPS - 2):
        got = exchanged(step(got, hot[0], by_col, devices))
        got = exchanged(step(got, hot[1], by_row, devices))
    last = exchanged(last_step(at_core, at_chip, slots, got, hot[0], by_col, devices))
    got, last = tied((got, last))
    logs = [jax.ShapeDtypeStruct((blocks_dev * TILES, LANES), f32)] * 2
    row_log, col_log = on_chip(log_kernel, logs, 2**20, (got, hot[2], last, hot[3]))
    return row_log.reshape(-1), col_log.reshape(-1)


def solution(mesh):
    torus = Mesh(mesh.devices.reshape(4, 2, 4, 4), ("aa_0", "aa_1", "ba_0", "ba_1"))
    in_specs = (P(BA, AA), P(BA, AA), P(), P(), P(BA, None, None))
    out_specs = (P(BA), P(BA))
    return jax.shard_map(
        per_device, mesh=torus, in_specs=in_specs, out_specs=out_specs, check_vma=False
    )
```
